32 devices in a mesh: g: 32 (over z, y, x, core).
Axes of the slice: x: 2, y: 2, z: 4, core: 2. Of those that a mesh axis runs over, the one named last changes fastest.
Arguments:
- features: bfloat16 [65536, 128], P(None, 'g')
- w_self1: bfloat16 [128, 128], P('g')
- w_nbr1: bfloat16 [128, 128], P('g')
- nbr_ids: int32 [65536, 10], P('g')
- nbr_mask: int32 [65536, 10], P('g')
- w_self2: bfloat16 [128, 128], replicated
- w_nbr2: bfloat16 [128, 128], replicated
- w_self3: bfloat16 [128, 40], replicated
- w_nbr3: bfloat16 [128, 40], replicated
- labels: int32 [65536], P('g')
Outputs:
- output 1: float32 [], replicated
- output 2: float32 [128, 128], P('g')
- output 3: float32 [128, 128], P('g')
- output 4: float32 [128, 128], replicated
- output 5: float32 [128, 128], replicated
- output 6: float32 [128, 40], replicated
- output 7: float32 [128, 40], replicated
All inputs are finite; a program needn't handle non-finite values.
Results may differ from the reference program's by a relative error of at most 0.00265331.
Values are sent between devices in bfloat16 or wider.
A program may use at most 1 GiB of HBM per device.

```python
import jax
import jax.numpy as jnp
from jax import lax

NUM_NODES = 65536
FEAT_DIM = 128
HID_DIM = 128
NUM_CLASSES = 40
FAN_IN = 10


def draw_graph(key):
    key_perm, key_pos, key_one, key_two, key_keep = jax.random.split(key, 5)
    node_perm = jax.random.permutation(key_perm, NUM_NODES).astype(jnp.int32)
    slot_pos = jax.random.randint(key_pos, (NUM_NODES, 1), 0, FAN_IN)
    draw_one = jax.random.randint(key_one, (NUM_NODES, FAN_IN), 0, NUM_NODES)
    draw_two = jax.random.randint(key_two, (NUM_NODES, FAN_IN), 0, NUM_NODES)
    slot_ids = jnp.arange(FAN_IN)[None, :]
    row_ids = jnp.arange(NUM_NODES)[:, None]
    at_pos = slot_ids == slot_pos
    nbr_ids = jnp.where(at_pos, node_perm[:, None], jnp.minimum(draw_one, draw_two)).astype(jnp.int32)
    keep = jax.random.randint(key_keep, (NUM_NODES, FAN_IN), 0, 4) > 0
    valid = at_pos | (keep & (row_ids != 1)) | (row_ids == 0)
    return nbr_ids, valid.astype(jnp.int32)


def setup_inputs(seed: int = 0) -> dict:
    keys = jax.random.split(jax.random.key(seed), 10)

    def weight(key, fan_rows, fan_cols, gain):
        scale = gain / fan_rows ** 0.5
        return (jax.random.normal(key, (fan_rows, fan_cols), jnp.float32) * scale).astype(jnp.bfloat16)

    nbr_ids, nbr_mask = draw_graph(keys[3])
    return dict(
        features=jax.random.normal(keys[0], (NUM_NODES, FEAT_DIM), jnp.float32).astype(jnp.bfloat16),
        w_self1=weight(keys[1], FEAT_DIM, HID_DIM, 1.0),
        w_nbr1=weight(keys[2], FEAT_DIM, HID_DIM, 2.0),
        nbr_ids=nbr_ids,
        nbr_mask=nbr_mask,
        w_self2=weight(keys[4], HID_DIM, HID_DIM, 1.0),
        w_nbr2=weight(keys[5], HID_DIM, HID_DIM, 2.0),
        w_self3=weight(keys[6], HID_DIM, NUM_CLASSES, 1.0),
        w_nbr3=weight(keys[7], HID_DIM, NUM_CLASSES, 2.0),
        labels=jax.random.randint(keys[8], (NUM_NODES,), 0, NUM_CLASSES).astype(jnp.int32),
    )


def neighbour_mean(table, nbr_ids, mask_f, degree):
    table_f = table.astype(jnp.float32)

    def body(running, slot_cols):
        ids_k, wts_k = slot_cols
        return running + wts_k[:, None] * table_f[ids_k], None

    start = jnp.zeros((nbr_ids.shape[0], table.shape[1]), jnp.float32)
    total, _ = lax.scan(body, start, (nbr_ids.T, mask_f.T))
    return total / degree[:, None]


def neighbour_mean_t(grads, nbr_ids, mask_f, degree):
    scaled = grads.astype(jnp.float32) / degree[:, None]

    def body(running, slot_cols):
        ids_k, wts_k = slot_cols
        return running + jax.ops.segment_sum(wts_k[:, None] * scaled, ids_k, num_segments=NUM_NODES), None

    start = jnp.zeros((NUM_NODES, grads.shape[1]), jnp.float32)
    total, _ = lax.scan(body, start, (nbr_ids.T, mask_f.T))
    return total


def reference(features, w_self1, w_nbr1, nbr_ids, nbr_mask, w_self2, w_nbr2, w_self3, w_nbr3, labels):
    mask_f = nbr_mask.astype(jnp.float32)
    degree = jnp.sum(mask_f, axis=1)
    agg_x = neighbour_mean(features, nbr_ids, mask_f, degree).astype(jnp.bfloat16)
    pre_one = jnp.dot(features, w_self1, preferred_element_type=jnp.float32) + jnp.dot(agg_x, w_nbr1, preferred_element_type=jnp.float32)
    act_one = jnp.maximum(pre_one, 0.0).astype(jnp.bfloat16)
    agg_one = neighbour_mean(act_one, nbr_ids, mask_f, degree).astype(jnp.bfloat16)
    pre_two = jnp.dot(act_one, w_self2, preferred_element_type=jnp.float32) + jnp.dot(agg_one, w_nbr2, preferred_element_type=jnp.float32)
    act_two = jnp.maximum(pre_two, 0.0).astype(jnp.bfloat16)
    agg_two = neighbour_mean(act_two, nbr_ids, mask_f, degree).astype(jnp.bfloat16)
    logits = jnp.dot(act_two, w_self3, preferred_element_type=jnp.float32) + jnp.dot(agg_two, w_nbr3, preferred_element_type=jnp.float32)
    log_norm = jax.nn.logsumexp(logits, axis=1)
    onehot = (labels[:, None] == jnp.arange(NUM_CLASSES)[None, :]).astype(jnp.float32)
    mean_loss = jnp.sum(log_norm - jnp.sum(onehot * logits, axis=1)) / NUM_NODES
    g_three = ((jnp.exp(logits - log_norm[:, None]) - onehot) / NUM_NODES).astype(jnp.bfloat16)
    grad_self3 = jnp.dot(act_two.T, g_three, preferred_element_type=jnp.float32)
    grad_nbr3 = jnp.dot(agg_two.T, g_three, preferred_element_type=jnp.float32)
    d_agg_two = jnp.dot(g_three, w_nbr3.T, preferred_element_type=jnp.float32).astype(jnp.bfloat16)
    d_act_two = jnp.dot(g_three, w_self3.T, preferred_element_type=jnp.float32) + neighbour_mean_t(d_agg_two, nbr_ids, mask_f, degree)
    g_two = jnp.where(pre_two > 0, d_act_two, 0.0).astype(jnp.bfloat16)
    grad_self2 = jnp.dot(act_one.T, g_two, preferred_element_type=jnp.float32)
    grad_nbr2 = jnp.dot(agg_one.T, g_two, preferred_element_type=jnp.float32)
    d_agg_one = jnp.dot(g_two, w_nbr2.T, preferred_element_type=jnp.float32).astype(jnp.bfloat16)
    d_act_one = jnp.dot(g_two, w_self2.T, preferred_element_type=jnp.float32) + neighbour_mean_t(d_agg_one, nbr_ids, mask_f, degree)
    g_one = jnp.where(pre_one > 0, d_act_one, 0.0).astype(jnp.bfloat16)
    grad_self1 = jnp.dot(features.T, g_one, preferred_element_type=jnp.float32)
    grad_nbr1 = jnp.dot(agg_x.T, g_one, preferred_element_type=jnp.float32)
    return (mean_loss, grad_self1, grad_nbr1, grad_self2, grad_nbr2, grad_self3, grad_nbr3)
```

```python
import functools

import jax
import jax.numpy as jnp
from jax import lax
from jax.experimental import pallas as pl
from jax.experimental.pallas import tpu as pltpu
from jax.sharding import PartitionSpec as P

AX = 'g'
N = 65536
R = 2048
D = 128
K = 10
C = 40
NDEV = 32
NQ = 8
NBQ = 2
E = R * K
CAP = 2048
NACC = 8
MESH = pl.DeviceIdType.MESH
VMEM = pltpu.VMEM
BF = jnp.bfloat16
F32 = jnp.float32
VLIM = 62 * 1024 * 1024


def gather_blocks(x_ref, tab, lsem, rsem, ssem, csem, rb, arrived=None):
    cr = rb // NQ
    me = lax.axis_index(AX)
    z, y, x, c = me // 8, lax.rem(me // 4, 2), lax.rem(me // 2, 2), lax.rem(me, 2)

    def dev(z_, y_, x_, c_):
        return ((z_ * 2 + y_) * 2 + x_) * 2 + c_

    d_x, d_y, d_up, d_dn, d_c = dev(z, y, 1 - x, c), dev(z, 1 - y, x, c), me + 8, me - 8, dev(z, y, x, 1 - c)
    bar = pltpu.get_barrier_semaphore()
    for d in (d_x, d_y, d_c):
        pl.semaphore_signal(bar, inc=1, device_id=(d,), device_id_type=MESH)

    @pl.when(z < 3)
    def _():
        pl.semaphore_signal(bar, inc=1, device_id=(d_up,), device_id_type=MESH)

    @pl.when(z > 0)
    def _():
        pl.semaphore_signal(bar, inc=1, device_id=(d_dn,), device_id_type=MESH)

    pl.semaphore_wait(bar, 4 + lax.rem(z + 1, 4) // 2)

    def rows(zo, yo, xo, q):
        return pl.ds(pl.multiple_of(dev(zo, yo, xo, c) * rb + q * cr, cr), cr)

    def slot(zo, yo, xo, q):
        return ((zo * 2 + yo) * 2 + xo) * NQ + q

    def send(d, src, dst, ss, rs):
        pltpu.make_async_remote_copy(
            src_ref=src, dst_ref=dst, send_sem=ss, recv_sem=rs, device_id=(d,), device_id_type=MESH).start()

    def forward(zo, yo, xo, q, up, dn, to_x, to_y, src=None):
        dst = tab.at[rows(zo, yo, xo, q)]
        src = dst if src is None else src
        rs = rsem.at[slot(zo, yo, xo, q)]
        if up is not None:
            @pl.when(up)
            def _():
                send(d_up, src, dst, ssem.at[0], rs)

            @pl.when(dn)
            def _():
                send(d_dn, src, dst, ssem.at[1], rs)
        if to_x:
            send(d_x, src, dst, ssem.at[2], rs)
        if to_y:
            send(d_y, src, dst, ssem.at[3], rs)
        send(d_c, src, dst, csem.at[0], csem.at[1])

    for q in range(NQ):
        forward(z, y, x, q, z < 3, z > 0, True, True, x_ref.at[pl.ds(q * cr, cr)])
    own = pltpu.make_async_copy(x_ref, tab.at[pl.ds(pl.multiple_of(me * rb, rb), rb)], lsem)
    own.start()
    zr = [z, z + 1 - 2 * lax.rem(z, 2), 2 - z // 2, 3 - 3 * (z // 2)]

    def handle(kind, r, q, first, par):
        zo = zr[r]
        yo = 1 - y if kind in 'YD' else y
        xo = 1 - x if kind in 'XD' else x
        here = tab.at[rows(zo, yo, xo, q)]
        pltpu.make_async_remote_copy(
            src_ref=here, dst_ref=here, send_sem=ssem.at[0], recv_sem=rsem.at[slot(zo, yo, xo, q)],
            device_id=(d_x,), device_id_type=MESH).wait_recv()
        up = dn = None
        if kind == 'C' or first:
            up, dn = (z < 3, z > 0) if r == 0 else ((zo < z) & (z < 3), (zo > z) & (z > 0))
        col = kind == 'C' and not first
        over = not first or r == 0
        forward(zo, yo, xo, q, up, dn,
                col or (kind == 'Y' and par == 1 and over), col or (kind == 'X' and par == 0 and over))
        if arrived is not None:
            arrived(dev(zo, yo, xo, c) * rb + q * cr, cr)

    for s in range(5):
        groups = []
        if s < 3:
            groups.append(('C', s + 1))
        if s < 4:
            groups += [('X', s), ('Y', s)]
        if s > 0:
            groups.append(('D', s - 1))
        for q in range(NBQ):
            for kind, r in groups:
                handle(kind, r, q, True, q % 2)

        def pair(p, _, groups=groups):
            for par in range(2):
                for kind, r in groups:
                    handle(kind, r, NBQ + 2 * p + par, False, par)
            return 0

        lax.fori_loop(0, (NQ - NBQ) // 2, pair, 0)

    def wait_chunks(n, sem):
        v = tab.at[pl.ds(0, n * cr)]
        pltpu.make_async_copy(v, v, sem).wait()

    own.wait()
    na = NQ - NBQ
    flat = 4 * na + 4 * (na // 2) + NBQ + NBQ // 2
    wait_chunks(flat, ssem.at[2])
    wait_chunks(flat, ssem.at[3])
    for k in range(3):
        @pl.when(z == k)
        def _(k=k):
            wait_chunks((k + 1) * (na + 4 * NBQ), ssem.at[0])

        @pl.when(z == 3 - k)
        def _(k=k):
            wait_chunks((k + 1) * (na + 4 * NBQ), ssem.at[1])
    wait_chunks(16 * NQ, csem.at[0])
    wait_chunks(16 * NQ, csem.at[1])


AG_SEMS = [pltpu.SemaphoreType.DMA, pltpu.SemaphoreType.DMA((16 * NQ,)), pltpu.SemaphoreType.DMA((4,)),
           pltpu.SemaphoreType.DMA((2,))]


def all_gather(v, cid, name):
    rb = v.shape[0]

    def kernel(x_ref, o_ref, lsem, rsem, ssem, csem):
        gather_blocks(x_ref, o_ref, lsem, rsem, ssem, csem, rb)

    return pl.pallas_call(
        kernel, out_shape=jax.ShapeDtypeStruct((rb * NDEV,) + v.shape[1:], v.dtype),
        in_specs=[pl.BlockSpec(memory_space=VMEM)], out_specs=pl.BlockSpec(memory_space=pl.ANY),
        scratch_shapes=AG_SEMS, name=name,
        compiler_params=pltpu.CompilerParams(collective_id=cid, has_side_effects=True))(v)


def dot(a, b):
    return jnp.dot(a, b, preferred_element_type=F32)


def dot_rows(a, b):
    return lax.dot_general(a, b, (((0,), (0,)), ((), ())), preferred_element_type=F32)


def dot_t(a, b):
    return lax.dot_general(a, b, (((1,), (1,)), ((), ())), preferred_element_type=F32)


CB = 256


def load_table(tab_hbm, tab, stg, tsem):
    nb, ch = stg.shape[0], stg.shape[1]

    def tcopy(i, s):
        return pltpu.make_async_copy(tab_hbm.at[pl.ds(pl.multiple_of(i * ch, ch), ch), :], stg.at[s], tsem.at[s])

    for s in range(nb - 1):
        tcopy(s, s).start()

    def conv(i, _):
        s = lax.rem(i, nb)
        tcopy(i, s).wait()

        @pl.when(i + nb - 1 < N // ch)
        def _():
            tcopy(i + nb - 1, lax.rem(i + nb - 1, nb)).start()

        tab[pl.ds(pl.multiple_of(i * ch, ch), ch), :] = stg[s].astype(F32)
        return 0

    lax.fori_loop(0, N // ch, conv, 0)


def table_mean(tab_hbm, idx_ref, tab, stg, acc, tsem):
    load_table(tab_hbm, tab, stg, tsem)
    tab[pl.ds(N, 8), :] = jnp.zeros((8, D), F32)

    def body(b, _):
        for u in range(8):
            r = b * 8 + u
            v = [tab[pl.ds(idx_ref[k * R + r], 1), :] for k in range(K)]
            while len(v) > 1:
                v = [v[j] + v[j + 1] if j + 1 < len(v) else v[j] for j in range(0, len(v), 2)]
            acc[pl.ds(r, 1), :] = v[0]
        return 0

    lax.fori_loop(0, R // 8, body, 0)


TABLE = [VMEM((N + 8, D), F32), VMEM((4, 1024, D), BF), VMEM((R, D), F32), pltpu.SemaphoreType.DMA((4,))]


def hidden_layer(v, idx, deg, w_self, w_nbr, name):
    def kernel(idx_ref, tab_hbm, x_ref, deg_ref, ws_ref, wn_ref, agg_ref, pre_ref, act_ref, tab, stg, acc, tsem):
        table_mean(tab_hbm, idx_ref, tab, stg, acc, tsem)

        def block(i, _):
            r = pl.ds(pl.multiple_of(i * CB, CB), CB)
            agg = (acc[r, :] / deg_ref[r, :]).astype(BF)
            agg_ref[r, :] = agg
            pre = dot(x_ref[r, :], ws_ref[...]) + dot(agg, wn_ref[...])
            pre_ref[r, :] = pre
            act_ref[r, :] = jnp.maximum(pre, 0.0).astype(BF)
            return 0

        lax.fori_loop(0, R // CB, block, 0)

    vm = pl.BlockSpec(memory_space=VMEM)
    return pl.pallas_call(
        kernel, name=name,
        out_shape=[jax.ShapeDtypeStruct((R, D), BF), jax.ShapeDtypeStruct((R, D), F32), jax.ShapeDtypeStruct((R, D), BF)],
        in_specs=[pl.BlockSpec(memory_space=pltpu.SMEM), pl.BlockSpec(memory_space=pl.ANY), vm, vm, vm, vm],
        out_specs=[vm] * 3, scratch_shapes=TABLE, compiler_params=pltpu.CompilerParams(vmem_limit_bytes=VLIM),
    )(idx, all_gather(v, 2, 'gather_rows'), v, deg, w_self, w_nbr)


def output_layer(v, idx, deg, labels, w_self, w_nbr, name):
    def kernel(idx_ref, tab_hbm, x_ref, deg_ref, lab_ref, ws_ref, wn_ref, g_ref, u_ref, dws_ref, dwn_ref, loss_ref,
               tab, stg, acc, tsem):
        table_mean(tab_hbm, idx_ref, tab, stg, acc, tsem)
        dws_ref[...] = jnp.zeros((D, D), F32)
        dwn_ref[...] = jnp.zeros((D, D), F32)
        lane = lax.broadcasted_iota(jnp.int32, (CB, D), 1)

        def block(i, loss):
            r = pl.ds(pl.multiple_of(i * CB, CB), CB)
            act = x_ref[r, :]
            agg = (acc[r, :] / deg_ref[r, :]).astype(BF)
            logits = dot(act, ws_ref[...]) + dot(agg, wn_ref[...])
            live = lane < C
            top = jnp.max(jnp.where(live, logits, -jnp.inf), axis=1, keepdims=True)
            ex = jnp.where(live, jnp.exp(logits - top), 0.0)
            norm = top + jnp.log(jnp.sum(ex, axis=1, keepdims=True))
            hot = jnp.where(lane == lab_ref[r, :], 1.0, 0.0)
            loss = loss + jnp.sum(jnp.where(live, hot * (norm - logits), 0.0))
            prob = jnp.where(live, jnp.exp(logits - norm), 0.0)
            g = ((prob - hot) / N).astype(BF)
            g_ref[r, :] = g
            u_ref[r, :] = dot_t(g, wn_ref[...]).astype(BF)
            dws_ref[...] += dot_rows(act, g)
            dwn_ref[...] += dot_rows(agg, g)
            return loss

        loss = lax.fori_loop(0, R // CB, block, jnp.float32(0.0))
        loss_ref[...] = jnp.full((8, D), loss, F32)

    vm = pl.BlockSpec(memory_space=VMEM)
    return pl.pallas_call(
        kernel, name=name,
        out_shape=[jax.ShapeDtypeStruct((R, D), BF), jax.ShapeDtypeStruct((R, D), BF),
                   jax.ShapeDtypeStruct((D, D), F32), jax.ShapeDtypeStruct((D, D), F32), jax.ShapeDtypeStruct((8, D), F32)],
        in_specs=[pl.BlockSpec(memory_space=pltpu.SMEM), pl.BlockSpec(memory_space=pl.ANY)] + [vm] * 5,
        out_specs=[vm] * 5, scratch_shapes=TABLE, compiler_params=pltpu.CompilerParams(vmem_limit_bytes=VLIM),
    )(idx, all_gather(v, 2, 'gather_rows'), v, deg, labels, w_self, w_nbr)


def table_mean_t(lo_ref, hi_ref, src_hbm, dst_hbm, wt_hbm, tab_hbm, tab, stg, accs, lists, tsem, lsem):
    src, dst, wt = lists

    def list_copies(s, part, slot):
        off = pl.multiple_of(s * E + (lo_ref[s] // 1024) * 1024 + part * CAP, 1024)
        return [pltpu.make_async_copy(h.at[pl.ds(off, CAP)], b.at[pl.ds(pl.multiple_of(slot * CAP, CAP), CAP)], lsem.at[j, slot])
                for j, (h, b) in enumerate(((src_hbm, src), (dst_hbm, dst), (wt_hbm, wt)))]

    for cp in list_copies(0, 0, 0):
        cp.start()

    load_table(tab_hbm, tab, stg, tsem)
    for a in accs:
        a[...] = jnp.zeros(a.shape, F32)

    def run(slot, first, last):
        def body(b, _):
            for u in range(NACC):
                e = slot * CAP + b * NACC + u
                d = pl.ds(dst[e], 1)
                accs[u][d, :] += tab[pl.ds(src[e], 1), :] * wt[e]
            return 0

        lax.fori_loop(first // NACC, (last + NACC - 1) // NACC, body, 0)

    def sender(s, _):
        slot = lax.rem(s, 2)
        for cp in list_copies(s, 0, slot):
            cp.wait()

        @pl.when(s + 1 < NDEV)
        def _():
            for cp in list_copies(s + 1, 0, 1 - slot):
                cp.start()

        base = (lo_ref[s] // 1024) * 1024
        run(slot, lo_ref[s] - base, jnp.minimum(hi_ref[s] - base, CAP))

        def more(p, _):
            for cp in list_copies(s, p, slot):
                cp.start()
            for cp in list_copies(s, p, slot):
                cp.wait()
            run(slot, 0, jnp.minimum(hi_ref[s] - base - p * CAP, CAP))
            return 0

        lax.fori_loop(1, (hi_ref[s] - base + CAP - 1) // CAP, more, 0)
        return 0

    lax.fori_loop(0, NDEV, sender, 0)


def backward_layer(table, lo, hi, lists, g_up, w_self, pre, act, agg, w_nbr, name):
    last = w_nbr is None

    def kernel(lo_ref, hi_ref, src_hbm, dst_hbm, wt_hbm, tab_hbm, gu_ref, ws_ref, pre_ref, act_ref, agg_ref, *rest):
        if last:
            dws_ref, dwn_ref = rest[:2]
            rest = rest[2:]
        else:
            wn_ref, g_ref, u_ref, dws_ref, dwn_ref = rest[:5]
            rest = rest[5:]
        tab, stg = rest[:2]
        accs = rest[2:2 + NACC]
        src, dst, wt, tsem, lsem = rest[2 + NACC:]
        table_mean_t(lo_ref, hi_ref, src_hbm, dst_hbm, wt_hbm, tab_hbm, tab, stg, accs, (src, dst, wt), tsem, lsem)
        dws_ref[...] = jnp.zeros((D, D), F32)
        dwn_ref[...] = jnp.zeros((D, D), F32)

        def block(i, _):
            r = pl.ds(pl.multiple_of(i * CB, CB), CB)
            back = [a[r, :] for a in accs]
            while len(back) > 1:
                back = [back[j] + back[j + 1] for j in range(0, len(back), 2)]
            d_act = dot_t(gu_ref[r, :], ws_ref[...]) + back[0]
            g = jnp.where(pre_ref[r, :] > 0, d_act, 0.0).astype(BF)
            dws_ref[...] += dot_rows(act_ref[r, :], g)
            dwn_ref[...] += dot_rows(agg_ref[r, :], g)
            if not last:
                g_ref[r, :] = g
                u_ref[r, :] = dot_t(g, wn_ref[...]).astype(BF)
            return 0

        lax.fori_loop(0, R // CB, block, 0)

    vm, sm, hb = (pl.BlockSpec(memory_space=m) for m in (VMEM, pltpu.SMEM, pl.ANY))
    outs = [jax.ShapeDtypeStruct((D, D), F32)] * 2
    args = [lo, hi, *lists, table, g_up, w_self, pre, act, agg]
    specs = [sm, sm, hb, hb, hb, hb, vm, vm, vm, vm, vm]
    if not last:
        outs = [jax.ShapeDtypeStruct((R, D), BF)] * 2 + outs
        args.append(w_nbr)
        specs.append(vm)
    return pl.pallas_call(
        kernel, name=name, out_shape=outs, in_specs=specs, out_specs=[vm] * len(outs),
        scratch_shapes=[VMEM((N, D), F32), VMEM((4, 1024, D), BF)] + [VMEM((R + 8, D), F32)] * NACC
        + [pltpu.SMEM((2 * CAP,), jnp.int32), pltpu.SMEM((2 * CAP,), jnp.int32), pltpu.SMEM((2 * CAP,), F32),
           pltpu.SemaphoreType.DMA((4,)), pltpu.SemaphoreType.DMA((3, 2))],
        compiler_params=pltpu.CompilerParams(vmem_limit_bytes=VLIM))(*args)


def in_edges(nbr_t, mask_t, deg, cid):
    me = lax.axis_index(AX)
    live = mask_t > 0
    here = jnp.arange(R, dtype=jnp.int32)[None, :]
    key = jnp.where(live, nbr_t * 32768 + here * 16 + deg[None, :], -1)
    key = lax.sort(key.reshape(E))
    bounds = jnp.arange(NDEV + 1, dtype=jnp.int32)
    starts = jnp.sum(((key >> 26)[None, :] < bounds[:, None]).astype(jnp.int32), axis=1)
    pay = jnp.concatenate([key.reshape(E // D, D), jnp.pad(starts[None, :], ((0, 31), (0, D - NDEV - 1)))])
    every = all_gather(pay, cid, 'gather_edges').reshape(NDEV, E // D + 32, D)
    keys = every[:, :E // D].reshape(NDEV, E)
    sender = jnp.arange(NDEV, dtype=jnp.int32)[:, None]
    src = ((keys >> 4) & (R - 1)) + sender * R
    dst = (keys >> 15) - me * R
    dst = jnp.where((dst < 0) | (dst >= R) | (keys < 0), R, dst)
    wt = 1.0 / jnp.maximum(keys & 15, 1).astype(F32)
    pad = lambda v: jnp.pad(v.reshape(-1), (0, CAP))
    marks = every[:, E // D, :NDEV + 1]
    lo = lax.dynamic_index_in_dim(marks, me, 1, keepdims=False)
    hi = lax.dynamic_index_in_dim(marks, me + 1, 1, keepdims=False)
    return lo, hi, (pad(src), pad(dst), pad(wt))


RED = 24


def reduce_shares(parts, cid):
    def kernel(p_ref, own_ref, all_ref, got, mine, rsem, ssem, lsem):
        me = lax.axis_index(AX)
        bar = pltpu.get_barrier_semaphore()

        def greet(k, _):
            pl.semaphore_signal(bar, inc=1, device_id=(lax.rem(me + k, NDEV),), device_id_type=MESH)
            return 0

        lax.fori_loop(1, NDEV, greet, 0)
        pl.semaphore_wait(bar, NDEV - 1)

        def share(k, _):
            d = lax.rem(me + k, NDEV)
            pltpu.make_async_remote_copy(
                src_ref=p_ref.at[d], dst_ref=got.at[me], send_sem=ssem.at[0], recv_sem=rsem.at[0],
                device_id=(d,), device_id_type=MESH).start()
            return 0

        lax.fori_loop(1, NDEV, share, 0)
        own = pltpu.make_async_copy(p_ref.at[me], got.at[me], lsem.at[0])
        own.start()
        own.wait()
        most = got.at[pl.ds(0, NDEV - 1)]
        pltpu.make_async_copy(most, most, rsem.at[0]).wait()
        v = [got[d] for d in range(NDEV)]
        while len(v) > 1:
            v = [v[j] + v[j + 1] for j in range(0, len(v), 2)]
        own_ref[...] = v[0][:8]
        mine[...] = v[0][8:]

        def tell(k, _):
            d = lax.rem(me + k, NDEV)
            pltpu.make_async_remote_copy(
                src_ref=mine, dst_ref=all_ref.at[me], send_sem=ssem.at[1], recv_sem=rsem.at[1],
                device_id=(d,), device_id_type=MESH).start()
            return 0

        lax.fori_loop(1, NDEV, tell, 0)
        keep = pltpu.make_async_copy(mine, all_ref.at[me], lsem.at[1])
        keep.start()
        keep.wait()
        most = all_ref.at[pl.ds(0, NDEV - 1)]
        pltpu.make_async_copy(most, most, rsem.at[1]).wait()
        pltpu.make_async_copy(most, most, ssem.at[1]).wait()
        most = got.at[pl.ds(0, NDEV - 1)]
        pltpu.make_async_copy(most, most, ssem.at[0]).wait()

    vm = pl.BlockSpec(memory_space=VMEM)
    return pl.pallas_call(
        kernel, name='reduce_shares',
        out_shape=[jax.ShapeDtypeStruct((8, D), F32), jax.ShapeDtypeStruct((NDEV, RED - 8, D), F32)],
        in_specs=[vm], out_specs=[vm, vm],
        scratch_shapes=[VMEM((NDEV, RED, D), F32), VMEM((RED - 8, D), F32)] + [pltpu.SemaphoreType.DMA((2,))] * 3,
        compiler_params=pltpu.CompilerParams(collective_id=cid, has_side_effects=True))(parts)


def solution(mesh):
    def device_step(feat_cols, w_self1_rows, w_nbr1_rows, nbr_rows, mask_rows, w_self2, w_nbr2, w_self3, w_nbr3, label_rows):
        nbr_t, mask_t = nbr_rows.T, mask_rows.T
        deg = jnp.sum(mask_t, axis=0)
        deg_wide = jnp.broadcast_to(deg.astype(F32)[:, None], (R, D))
        idx = jnp.where(mask_t > 0, nbr_t, N).reshape(E)
        w1_rows = jnp.concatenate([w_self1_rows, w_nbr1_rows], axis=1)
        out_going = jnp.concatenate(
            [feat_cols.T.reshape(4, NDEV, R), jnp.broadcast_to(w1_rows[:, None, :], (4, NDEV, 2 * D))], axis=2)
        in_coming = lax.all_to_all(out_going, AX, 1, 0, tiled=True).reshape(D, R + 2 * D)
        feat = in_coming[:, :R].T
        w_self1, w_nbr1 = in_coming[:, R:R + D], in_coming[:, R + D:]
        lo, hi, lists = in_edges(nbr_t, mask_t, deg, 1)
        wide = lambda w: jnp.pad(w, ((0, 0), (0, D - C)))
        ws3, wn3 = wide(w_self3), wide(w_nbr3)
        agg_x, pre_one, act_one = hidden_layer(feat, idx, deg_wide, w_self1, w_nbr1, 'layer_one')
        agg_one, pre_two, act_two = hidden_layer(act_one, idx, deg_wide, w_self2, w_nbr2, 'layer_two')
        g_three, u_two, dws3, dwn3, loss = output_layer(
            act_two, idx, deg_wide, label_rows[:, None], ws3, wn3, 'layer_three')
        g_two, u_one, dws2, dwn2 = backward_layer(
            all_gather(u_two, 2, 'gather_rows'), lo, hi, lists, g_three, ws3, pre_two, act_one, agg_one, w_nbr2, 'back_two')
        dws1, dwn1 = backward_layer(
            all_gather(u_one, 2, 'gather_rows'), lo, hi, lists, g_two, w_self2, pre_one, feat, agg_x, None, 'back_one')
        cut = lambda v: v.reshape(NDEV, D // NDEV, D)
        last = jnp.concatenate([dws3[:, :D // 2], dwn3[:, :D // 2]], axis=1)
        parts = jnp.concatenate(
            [cut(v) for v in (dws1, dwn1, dws2, dwn2, last)] + [jnp.broadcast_to(loss[None, :4], (NDEV, 4, D))], axis=1)
        own, every = reduce_shares(parts, 7)
        whole = lambda j: every[:, j:j + 4].reshape(D, D)
        last = whole(8)
        return (every[0, 12, 0] / N, own[:4], own[4:], whole(0), whole(4), last[:, :C], last[:, D // 2:D // 2 + C])

    row = P(AX, None)
    return jax.shard_map(
        device_step, mesh=mesh,
        in_specs=(P(None, AX), row, row, row, row, P(), P(), P(), P(), P(AX)),
        out_specs=(P(), row, row, P(), P(), P(), P()),
        check_vma=False)
```

```python
import functools

import jax
import jax.numpy as jnp
from jax import lax
from jax.experimental import pallas as pl
from jax.experimental.pallas import tpu as pltpu
from jax.sharding import PartitionSpec as P

AX = 'g'
N = 65536
R = 2048
D = 128
K = 10
C = 40
NDEV = 32
E = R * K
CAP = 2048
NACC = 16
SLOTS = 8
TCH = 2048
TBUF = 6
MESH = pl.DeviceIdType.MESH
VMEM = pltpu.VMEM
BF = jnp.bfloat16
F32 = jnp.float32
VLIM = 62 * 1024 * 1024


def gather_blocks(arrays, chunks, order, lsem, rsem, sems):
    nq = len(chunks)
    me = lax.axis_index(AX)
    z, y, x, c = me // 8, lax.rem(me // 4, 2), lax.rem(me // 2, 2), lax.rem(me, 2)

    def dev(z_, y_, x_, c_):
        return ((z_ * 2 + y_) * 2 + x_) * 2 + c_

    d_x, d_y, d_up, d_dn, d_c = dev(z, y, 1 - x, c), dev(z, 1 - y, x, c), me + 8, me - 8, dev(z, y, x, 1 - c)
    bar = pltpu.get_barrier_semaphore()
    for d in (d_x, d_y, d_c):
        pl.semaphore_signal(bar, device_id=(d,), device_id_type=MESH)

    @pl.when(z < 3)
    def _():
        pl.semaphore_signal(bar, device_id=(d_up,), device_id_type=MESH)

    @pl.when(z > 0)
    def _():
        pl.semaphore_signal(bar, device_id=(d_dn,), device_id_type=MESH)

    pl.semaphore_wait(bar, 4 + lax.rem(z + 1, 4) // 2)
    sent = [[[0] for _ in range(4)] for _ in arrays]

    def place(q, zo, yo, xo):
        array, first, rows, _ = chunks[q]
        block, table = arrays[array]
        return table.at[pl.ds(pl.multiple_of(dev(zo, yo, xo, c) * block.shape[0] + first, 8), rows)]

    def slot(q, zo, yo, xo):
        return rsem.at[((zo * 2 + yo) * 2 + xo) * nq + q]

    def forward(q, zo, yo, xo, up, dn, to_x, to_y, src=None):
        dst = place(q, zo, yo, xo)
        src = dst if src is None else src
        ssem, csem = sems[chunks[q][0]]

        def send(d, ss, rs):
            pltpu.make_async_remote_copy(
                src_ref=src, dst_ref=dst, send_sem=ss, recv_sem=rs, device_id=(d,), device_id_type=MESH).start()

        if up is not None:
            @pl.when(up)
            def _():
                send(d_up, ssem.at[0], slot(q, zo, yo, xo))

            @pl.when(dn)
            def _():
                send(d_dn, ssem.at[1], slot(q, zo, yo, xo))
        for there, d, j in ((to_x, d_x, 2), (to_y, d_y, 3)):
            if there:
                send(d, ssem.at[j], slot(q, zo, yo, xo))
                sent[chunks[q][0]][j][0] += chunks[q][2]
        send(d_c, csem.at[0], csem.at[1])

    own = []
    for q in order[:nq]:
        array, first, rows, _ = chunks[q]
        forward(q, z, y, x, z < 3, z > 0, True, True, arrays[array][0].at[pl.ds(first, rows)])
    for j, (block, table) in enumerate(arrays):
        rb = block.shape[0]
        own.append(pltpu.make_async_copy(block, table.at[pl.ds(pl.multiple_of(me * rb, 8), rb)], lsem.at[j]))
        own[j].start()
    zr = [z, z + 1 - 2 * lax.rem(z, 2), 2 - z // 2, 3 - 3 * (z // 2)]

    for code in order[nq:]:
        kind, r, q = code // 100, code // 10 % 10, code % 10
        plane_first = chunks[q][3]
        zo, yo, xo = zr[r], 1 - y if kind >= 2 else y, 1 - x if kind % 2 else x
        here = place(q, zo, yo, xo)
        pltpu.make_async_remote_copy(
            src_ref=here, dst_ref=here, send_sem=sems[0][0].at[0], recv_sem=slot(q, zo, yo, xo),
            device_id=(d_x,), device_id_type=MESH).wait_recv()
        up = dn = None
        if kind == 0 or plane_first:
            up, dn = (z < 3, z > 0) if r == 0 else ((zo < z) & (z < 3), (zo > z) & (z > 0))
        column = kind == 0 and not plane_first
        across = not plane_first or r == 0
        forward(q, zo, yo, xo, up, dn,
                column or (kind == 2 and q % 2 == 1 and across), column or (kind == 1 and q % 2 == 0 and across))

    for j, (block, table) in enumerate(arrays):
        ssem, csem = sems[j]

        def wait_rows(n, sem, table=table):
            v = table.at[pl.ds(0, n)]
            pltpu.make_async_copy(v, v, sem).wait()

        own[j].wait()
        for k in (2, 3):
            wait_rows(sent[j][k][0], ssem.at[k])
        step = sum(rows * (4 if plane_first else 1) for array, _, rows, plane_first in chunks if array == j)
        for k in range(3):
            @pl.when(z == k)
            def _(k=k):
                wait_rows((k + 1) * step, ssem.at[0])

            @pl.when(z == 3 - k)
            def _(k=k):
                wait_rows((k + 1) * step, ssem.at[1])
        wait_rows(16 * block.shape[0], csem.at[0])
        wait_rows(16 * block.shape[0], csem.at[1])


def cut(*sizes, array=0, plane_first=0):
    return [(array, sum(sizes[:i]), n, i < plane_first) for i, n in enumerate(sizes)]


def steps(*words):
    every = [w // 1000 ** i % 1000 for w in words for i in reversed(range(8))]
    return [v for v in every if v != 999]


ROW_CHUNKS = cut(224, 224, 272, 272, 272, 272, 256, 256, plane_first=2)
ROW_ORDER = steps(
    2003006005000004001007, 14100013201206200204016, 12017027023207101116026, 25015036111032033034211,
    24035021213020115215106, 300110022037220125126205, 104225320113112316120136, 224102217130310203011124,
    301227234114235105132237, 135307313212122010236117, 31134210107123216315121, 202223131103127306321311,
    304030317233133222312232, 137221231326331226230302, 303214305330336332322333, 323337325335314327334324)
PACKED_CHUNKS = cut(112, 112, 144, 144, 128, 128, 128, 128, plane_first=2) + cut(168, array=1)
PACKED_ORDER = list(range(9)) + [
    kind * 100 + (s + step) * 10 + q for s in range(5) for q in range(9)
    for kind, step in ((0, 1), (1, 0), (2, 0), (3, -1)) if 0 <= s + step <= 3]


def all_gather(blocks, chunks, order, cid, name):
    n = len(blocks)

    def kernel(*refs):
        lsem, rsem, *sems = refs[2 * n:]
        gather_blocks(list(zip(refs[:n], refs[n:2 * n])), chunks, order, lsem, rsem, list(zip(sems[::2], sems[1::2])))

    dma = pltpu.SemaphoreType.DMA
    return pl.pallas_call(
        kernel, out_shape=[jax.ShapeDtypeStruct((v.shape[0] * NDEV,) + v.shape[1:], v.dtype) for v in blocks],
        in_specs=[pl.BlockSpec(memory_space=VMEM)] * n, out_specs=[pl.BlockSpec(memory_space=pl.ANY)] * n,
        scratch_shapes=[dma((n,)), dma((16 * len(chunks),))] + [dma((4,)), dma((2,))] * n, name=name,
        compiler_params=pltpu.CompilerParams(collective_id=cid, has_side_effects=True))(*blocks)


def gather_rows(v):
    return all_gather([v], ROW_CHUNKS, ROW_ORDER, 2, 'gather_rows')[0]


def dot(a, b):
    return jnp.dot(a, b, preferred_element_type=F32)


def dot_rows(a, b):
    return lax.dot_general(a, b, (((0,), (0,)), ((), ())), preferred_element_type=F32)


def dot_t(a, b):
    return lax.dot_general(a, b, (((1,), (1,)), ((), ())), preferred_element_type=F32)


CB = 256


def load_table(tab_hbm, tab, stg, tsem, w_ref=None, meanwhile=None):
    nb, ch = stg.shape[0], stg.shape[1] if w_ref is None else HALF
    stg = stg if w_ref is None else stg.at[:, pl.ds(0, HALF)]
    count = N // ch if w_ref is None else N // R

    def tcopy(i, s):
        return pltpu.make_async_copy(tab_hbm.at[pl.ds(pl.multiple_of(i * ch, ch), ch), :], stg.at[s], tsem.at[s])

    for s in range(nb - 1):
        tcopy(s, s).start()
    if meanwhile is not None:
        meanwhile()

    def conv(i, _):
        s = lax.rem(i, nb)
        tcopy(i, s).wait()

        @pl.when(i + nb - 1 < count)
        def _():
            tcopy(i + nb - 1, lax.rem(i + nb - 1, nb)).start()

        if w_ref is None:
            tab[pl.ds(pl.multiple_of(i * ch, ch), ch), :] = stg[s].astype(F32)
        else:
            for half in range(2):
                for q in range(HALF // CB):
                    r = pl.ds(pl.multiple_of(i * R + half * HALF + q * CB, CB), CB)
                    tab[r, :] = dot_t(stg[s, q * CB:(q + 1) * CB, :], w_ref[half]).astype(BF).astype(F32)
        return 0

    lax.fori_loop(0, count, conv, 0)


def table_mean(tab_hbm, idx_ref, tab, stg, acc, tsem):
    load_table(tab_hbm, tab, stg, tsem)
    tab[pl.ds(N, 8), :] = jnp.zeros((8, D), F32)

    def body(b, _):
        for u in range(8):
            r = b * 8 + u
            v = [tab[pl.ds(idx_ref[k * R + r], 1), :] for k in range(K)]
            while len(v) > 1:
                v = [v[j] + v[j + 1] if j + 1 < len(v) else v[j] for j in range(0, len(v), 2)]
            acc[pl.ds(r, 1), :] = v[0]
        return 0

    lax.fori_loop(0, R // 8, body, 0)


TABLE = [VMEM((N + 8, D), F32), VMEM((TBUF, TCH, D), BF), VMEM((R, D), F32), pltpu.SemaphoreType.DMA((TBUF,))]


def hidden_layer(v, idx, deg, w_self, w_nbr, name):
    def kernel(idx_ref, tab_hbm, x_ref, deg_ref, ws_ref, wn_ref, agg_ref, pre_ref, act_ref, tab, stg, acc, tsem):
        table_mean(tab_hbm, idx_ref, tab, stg, acc, tsem)

        def block(i, _):
            r = pl.ds(pl.multiple_of(i * CB, CB), CB)
            agg = (acc[r, :] / deg_ref[r, :]).astype(BF)
            agg_ref[r, :] = agg
            pre = dot(x_ref[r, :], ws_ref[...]) + dot(agg, wn_ref[...])
            pre_ref[r, :] = pre
            act_ref[r, :] = jnp.maximum(pre, 0.0).astype(BF)
            return 0

        lax.fori_loop(0, R // CB, block, 0)

    vm = pl.BlockSpec(memory_space=VMEM)
    return pl.pallas_call(
        kernel, name=name,
        out_shape=[jax.ShapeDtypeStruct((R, D), BF), jax.ShapeDtypeStruct((R, D), F32), jax.ShapeDtypeStruct((R, D), BF)],
        in_specs=[pl.BlockSpec(memory_space=pltpu.SMEM), pl.BlockSpec(memory_space=pl.ANY), vm, vm, vm, vm],
        out_specs=[vm] * 3, scratch_shapes=TABLE, compiler_params=pltpu.CompilerParams(vmem_limit_bytes=VLIM),
    )(idx, gather_rows(v), v, deg, w_self, w_nbr)


HALF = R // 2


def output_layer(v, idx, deg, labels, w_self, w_nbr, name):
    def kernel(idx_ref, tab_hbm, x_ref, deg_ref, lab_ref, ws_ref, wn_ref, g_ref, dws_ref, dwn_ref, loss_ref,
               tab, stg, acc, tsem):
        table_mean(tab_hbm, idx_ref, tab, stg, acc, tsem)
        dws_ref[...] = jnp.zeros((D, D), F32)
        dwn_ref[...] = jnp.zeros((D, D), F32)
        lane = lax.broadcasted_iota(jnp.int32, (CB, D), 1)

        def part(start, half):
            r = pl.ds(pl.multiple_of(start, CB), CB)
            act = x_ref[r, :]
            agg = (acc[r, :] / deg_ref[r, :]).astype(BF)
            logits = dot(act, ws_ref[half]) + dot(agg, wn_ref[half])
            col = lane - half * (D // 2)
            live = (col >= 0) & (col < C)
            top = jnp.max(jnp.where(live, logits, -jnp.inf), axis=1, keepdims=True)
            ex = jnp.where(live, jnp.exp(logits - top), 0.0)
            norm = top + jnp.log(jnp.sum(ex, axis=1, keepdims=True))
            hot = jnp.where(col == lab_ref[r, :], 1.0, 0.0)
            loss = jnp.sum(jnp.where(live, hot * (norm - logits), 0.0))
            prob = jnp.where(live, jnp.exp(logits - norm), 0.0)
            g = ((prob - hot) / N).astype(BF)
            dws_ref[...] += dot_rows(act, g)
            dwn_ref[...] += dot_rows(agg, g)
            return g, loss

        def block(i, loss):
            g_low, loss_low = part(i * CB, 0)
            g_high, loss_high = part(i * CB + HALF, 1)
            g_ref[pl.ds(pl.multiple_of(i * CB, CB), CB), :] = jnp.where(lane < D // 2, g_low, g_high)
            return loss + loss_low + loss_high

        loss = lax.fori_loop(0, HALF // CB, block, jnp.float32(0.0))
        loss_ref[...] = jnp.full((8, D), loss, F32)

    vm = pl.BlockSpec(memory_space=VMEM)
    return pl.pallas_call(
        kernel, name=name,
        out_shape=[jax.ShapeDtypeStruct((HALF, D), BF), jax.ShapeDtypeStruct((D, D), F32),
                   jax.ShapeDtypeStruct((D, D), F32), jax.ShapeDtypeStruct((8, D), F32)],
        in_specs=[pl.BlockSpec(memory_space=pltpu.SMEM), pl.BlockSpec(memory_space=pl.ANY)] + [vm] * 5,
        out_specs=[vm] * 4, scratch_shapes=TABLE, compiler_params=pltpu.CompilerParams(vmem_limit_bytes=VLIM),
    )(idx, gather_rows(v), v, deg, labels, w_self, w_nbr)


def table_mean_t(lo_ref, hi_ref, src_hbm, dst_hbm, wt_hbm, tab_hbm, tab, stg, accs, lists, tsem, lsem, wt_ref):
    src, dst, wt = lists

    def list_copies(s, part, slot):
        off = pl.multiple_of(s * SPAN + (lo_ref[s] // 1024) * 1024 + part * CAP, 1024)
        return [pltpu.make_async_copy(h.at[pl.ds(off, CAP)], b.at[pl.ds(pl.multiple_of(slot * CAP, CAP), CAP)], lsem.at[j, slot])
                for j, (h, b) in enumerate(((src_hbm, src), (dst_hbm, dst), (wt_hbm, wt)))]

    for s in range(SLOTS - 1):
        for cp in list_copies(s, 0, s):
            cp.start()

    def clear():
        for a in accs:
            a[...] = jnp.zeros(a.shape, F32)

    load_table(tab_hbm, tab, stg, tsem, wt_ref, clear)

    def run(slot, first, last):
        def body(b, _):
            for u in range(NACC):
                e = slot * CAP + b * NACC + u
                d = pl.ds(dst[e], 1)
                accs[u][d, :] += tab[pl.ds(src[e], 1), :] * wt[e]
            return 0

        lax.fori_loop(first // NACC, (last + NACC - 1) // NACC, body, 0)

    def sender(s, _):
        slot = lax.rem(s, SLOTS)
        for cp in list_copies(s, 0, slot):
            cp.wait()

        @pl.when(s + SLOTS - 1 < NDEV)
        def _():
            for cp in list_copies(s + SLOTS - 1, 0, lax.rem(s + SLOTS - 1, SLOTS)):
                cp.start()

        base = (lo_ref[s] // 1024) * 1024
        run(slot, lo_ref[s] - base, jnp.minimum(hi_ref[s] - base, CAP))

        def more(p, _):
            for cp in list_copies(s, p, slot):
                cp.start()
            for cp in list_copies(s, p, slot):
                cp.wait()
            run(slot, 0, jnp.minimum(hi_ref[s] - base - p * CAP, CAP))
            return 0

        lax.fori_loop(1, (hi_ref[s] - base + CAP - 1) // CAP, more, 0)
        return 0

    lax.fori_loop(0, NDEV, sender, 0)


def backward_layer(table, lo, hi, lists, g_up, w_self, pre, act, agg, w_nbr, w_up, name):
    last = w_up is None

    def kernel(lo_ref, hi_ref, src_hbm, dst_hbm, wt_hbm, tab_hbm, gu_ref, ws_ref, pre_ref, act_ref, agg_ref, *rest):
        wu_ref = None
        if last:
            dws_ref, dwn_ref = rest[:2]
            rest = rest[2:]
        else:
            wn_ref, wu_ref, g_ref, u_ref, dws_ref, dwn_ref = rest[:6]
            rest = rest[6:]
        tab, stg = rest[:2]
        accs = rest[2:2 + NACC]
        src, dst, wt, tsem, lsem = rest[2 + NACC:]
        table_mean_t(lo_ref, hi_ref, src_hbm, dst_hbm, wt_hbm, tab_hbm, tab, stg, accs, (src, dst, wt), tsem, lsem, wu_ref)
        dws_ref[...] = jnp.zeros((D, D), F32)
        dwn_ref[...] = jnp.zeros((D, D), F32)

        def part(start, up):
            r = pl.ds(pl.multiple_of(start, CB), CB)
            back = [a[r, :] for a in accs]
            while len(back) > 1:
                back = [back[j] + back[j + 1] for j in range(0, len(back), 2)]
            g = jnp.where(pre_ref[r, :] > 0, up + back[0], 0.0).astype(BF)
            dws_ref[...] += dot_rows(act_ref[r, :], g)
            dwn_ref[...] += dot_rows(agg_ref[r, :], g)
            if not last:
                g_ref[r, :] = g
                u_ref[r, :] = dot_t(g, wn_ref[...]).astype(BF)

        def block(i, _):
            if last:
                part(i * CB, dot_t(gu_ref[pl.ds(pl.multiple_of(i * CB, CB), CB), :], ws_ref[...]))
            else:
                gu = gu_ref[pl.ds(pl.multiple_of(i * CB, CB), CB), :]
                part(i * CB, dot_t(gu, ws_ref[0]))
                part(i * CB + HALF, dot_t(gu, ws_ref[1]))
            return 0

        lax.fori_loop(0, (R if last else HALF) // CB, block, 0)

    vm, sm, hb = (pl.BlockSpec(memory_space=m) for m in (VMEM, pltpu.SMEM, pl.ANY))
    outs = [jax.ShapeDtypeStruct((D, D), F32)] * 2
    args = [lo, hi, *lists, table, g_up, w_self, pre, act, agg]
    specs = [sm, sm, hb, hb, hb, hb, vm, vm, vm, vm, vm]
    if not last:
        outs = [jax.ShapeDtypeStruct((R, D), BF)] * 2 + outs
        args += [w_nbr, w_up]
        specs += [vm, vm]
    return pl.pallas_call(
        kernel, name=name, out_shape=outs, in_specs=specs, out_specs=[vm] * len(outs),
        scratch_shapes=[VMEM((N, D), F32), VMEM((TBUF, TCH, D), BF)] + [VMEM((R + 8, D), F32)] * NACC
        + [pltpu.SMEM((SLOTS * CAP,), jnp.int32), pltpu.SMEM((SLOTS * CAP,), jnp.int32), pltpu.SMEM((SLOTS * CAP,), F32),
           pltpu.SemaphoreType.DMA((TBUF,)), pltpu.SemaphoreType.DMA((3, SLOTS))],
        compiler_params=pltpu.CompilerParams(vmem_limit_bytes=VLIM))(*args)


def rank(j):
    return ((j >> 7) & (NDEV - 1)) * R + (j >> 12) * 128 + (j & 127)


SPAN = 21 * 1024


def sorted_edges(ids, live, deg):
    here = jnp.arange(R, dtype=jnp.int32)[None, :]
    key = jnp.where(live, ids * 32768 + here * 16 + deg[None, :], -1)
    key = lax.sort(key.reshape(E))
    bounds = jnp.arange(NDEV + 1, dtype=jnp.int32)
    starts = jnp.sum(((key >> 26)[None, :] < bounds[:, None]).astype(jnp.int32), axis=1)
    return jnp.concatenate([key.reshape(E // D, D), jnp.pad(starts[None, :], ((0, 7), (0, D - NDEV - 1)))])


def in_edges(every):
    me = lax.axis_index(AX)
    keys = every.reshape(NDEV, SPAN // D, D)
    sender = jnp.arange(NDEV, dtype=jnp.int32)[:, None, None]
    row = (keys >> 4) & (R - 1)
    src = rank(sender * R + row)
    dst = (keys >> 15) - me * R
    real = (dst >= 0) & (dst < R) & (keys >= 0) & (jnp.arange(SPAN // D)[None, :, None] < E // D)
    dst = jnp.where(real, dst, R)
    wt = 1.0 / jnp.maximum(keys & 15, 1).astype(F32)
    marks = keys[:, E // D, :NDEV + 1]
    lo = lax.dynamic_index_in_dim(marks, me, 1, keepdims=False)
    hi = lax.dynamic_index_in_dim(marks, me + 1, 1, keepdims=False)
    return lo, hi, (src.reshape(-1), dst.reshape(-1), wt.reshape(-1))


RED = 24


def reduce_shares(parts, cid):
    def kernel(p_ref, own_ref, all_ref, got, mine, rsem, ssem, lsem):
        me = lax.axis_index(AX)
        bar = pltpu.get_barrier_semaphore()

        def greet(k, _):
            pl.semaphore_signal(bar, device_id=(lax.rem(me + k, NDEV),), device_id_type=MESH)
            return 0

        lax.fori_loop(1, NDEV, greet, 0)
        pl.semaphore_wait(bar, NDEV - 1)

        def share(k, _):
            d = lax.rem(me + k, NDEV)
            pltpu.make_async_remote_copy(
                src_ref=p_ref.at[d], dst_ref=got.at[me], send_sem=ssem.at[0], recv_sem=rsem.at[0],
                device_id=(d,), device_id_type=MESH).start()
            return 0

        lax.fori_loop(1, NDEV, share, 0)
        own = pltpu.make_async_copy(p_ref.at[me], got.at[me], lsem.at[0])
        own.start()
        own.wait()
        most = got.at[pl.ds(0, NDEV - 1)]
        pltpu.make_async_copy(most, most, rsem.at[0]).wait()
        v = [got[d] for d in range(NDEV)]
        while len(v) > 1:
            v = [v[j] + v[j + 1] for j in range(0, len(v), 2)]
        own_ref[...] = v[0][:8]
        mine[...] = v[0][8:]

        def tell(k, _):
            d = lax.rem(me + k, NDEV)
            pltpu.make_async_remote_copy(
                src_ref=mine, dst_ref=all_ref.at[me], send_sem=ssem.at[1], recv_sem=rsem.at[1],
                device_id=(d,), device_id_type=MESH).start()
            return 0

        lax.fori_loop(1, NDEV, tell, 0)
        keep = pltpu.make_async_copy(mine, all_ref.at[me], lsem.at[1])
        keep.start()
        keep.wait()
        most = all_ref.at[pl.ds(0, NDEV - 1)]
        pltpu.make_async_copy(most, most, rsem.at[1]).wait()
        pltpu.make_async_copy(most, most, ssem.at[1]).wait()
        most = got.at[pl.ds(0, NDEV - 1)]
        pltpu.make_async_copy(most, most, ssem.at[0]).wait()

    vm = pl.BlockSpec(memory_space=VMEM)
    return pl.pallas_call(
        kernel, name='reduce_shares',
        out_shape=[jax.ShapeDtypeStruct((8, D), F32), jax.ShapeDtypeStruct((NDEV, RED - 8, D), F32)],
        in_specs=[vm], out_specs=[vm, vm],
        scratch_shapes=[VMEM((NDEV, RED, D), F32), VMEM((RED - 8, D), F32)] + [pltpu.SemaphoreType.DMA((2,))] * 3,
        compiler_params=pltpu.CompilerParams(collective_id=cid, has_side_effects=True))(parts)


def solution(mesh):
    def device_step(feat_cols, w_self1_rows, w_nbr1_rows, nbr_rows, mask_rows, w_self2, w_nbr2, w_self3, w_nbr3, label_rows):
        me = lax.axis_index(AX)
        live = mask_rows.T > 0
        ids = rank(nbr_rows.T)
        rows = jnp.concatenate([jnp.where(live, ids, N), label_rows[None, :], jnp.zeros((5, R), jnp.int32)])
        blocks = rows.reshape(16, 16, 128).transpose(1, 0, 2)
        blocks = lax.all_to_all(jnp.concatenate([blocks, blocks]), AX, 0, 0, tiled=True)
        rows = lax.dynamic_index_in_dim(blocks.reshape(16, 2, 16, 128), me // 16, 1, keepdims=False)
        rows = rows.transpose(1, 0, 2).reshape(16, R)
        idx, labels = rows[:K], rows[K]
        w1_rows = jnp.concatenate([w_self1_rows, w_nbr1_rows], axis=1)
        out_going = jnp.concatenate(
            [feat_cols.T.reshape(4, 16, NDEV, 128).transpose(2, 0, 1, 3).reshape(NDEV, 4, R),
             jnp.broadcast_to(w1_rows[None], (NDEV, 4, 2 * D))], axis=2)
        in_coming = lax.all_to_all(out_going, AX, 0, 0, tiled=True).reshape(D, R + 2 * D)
        feat = in_coming[:, :R].T
        w_self1, w_nbr1 = in_coming[:, R:R + D], in_coming[:, R + D:]
        edges = sorted_edges(ids, live, jnp.sum(mask_rows.T, axis=0))
        deg = jnp.sum((idx < N).astype(F32), axis=0)
        deg_wide = jnp.broadcast_to(deg[:, None], (R, D))
        idx = idx.reshape(E)
        halves = lambda w: jnp.stack([jnp.pad(w, ((0, 0), (0, D - C))), jnp.pad(w, ((0, 0), (D // 2, D // 2 - C)))])
        ws3, wn3 = halves(w_self3), halves(w_nbr3)
        agg_x, pre_one, act_one = hidden_layer(feat, idx, deg_wide, w_self1, w_nbr1, 'layer_one')
        agg_one, pre_two, act_two = hidden_layer(act_one, idx, deg_wide, w_self2, w_nbr2, 'layer_two')
        g_three, dws3, dwn3, loss = output_layer(act_two, idx, deg_wide, labels[:, None], ws3, wn3, 'layer_three')
        packed, edges = all_gather([g_three, edges], PACKED_CHUNKS, PACKED_ORDER, 5, 'gather_packed')
        lo, hi, lists = in_edges(edges)
        g_two, u_one, dws2, dwn2 = backward_layer(
            packed, lo, hi, lists, g_three, ws3, pre_two, act_one, agg_one, w_nbr2, wn3,
            'back_two')
        dws1, dwn1 = backward_layer(
            gather_rows(u_one), lo, hi, lists, g_two, w_self2, pre_one, feat, agg_x, None, None, 'back_one')
        cut = lambda v: v.reshape(NDEV, D // NDEV, D)
        last = jnp.concatenate([v[:, :D // 2] + v[:, D // 2:] for v in (dws3, dwn3)], axis=1)
        parts = jnp.concatenate(
            [cut(v) for v in (dws1, dwn1, dws2, dwn2, last)] + [jnp.broadcast_to(loss[None, :4], (NDEV, 4, D))], axis=1)
        own, every = reduce_shares(parts, 7)
        whole = lambda j: every[:, j:j + 4].reshape(D, D)
        last = whole(8)
        return (every[0, 12, 0] / N, own[:4], own[4:], whole(0), whole(4), last[:, :C], last[:, D // 2:D // 2 + C])

    row = P(AX, None)
    return jax.shard_map(
        device_step, mesh=mesh,
        in_specs=(P(None, AX), row, row, row, row, P(), P(), P(), P(), P(AX)),
        out_specs=(P(), row, row, P(), P(), P(), P()),
        check_vma=False)
```

```python
import jax
import jax.numpy as jnp
from jax import lax
from jax.experimental import pallas as pl
from jax.experimental.pallas import tpu as pltpu
from jax.sharding import PartitionSpec as P


AX = 'g'
N = 65536
R = 2048
D = 128
K = 10
C = 40
NDEV = 32
E = R * K
CAP = 2048
NACC = 16
EDGES = 32
SLOTS = 8
TBUF = 10
BBUF = 8
UNROLL = 16
MESH = pl.DeviceIdType.MESH
VMEM = pltpu.VMEM
BF = jnp.bfloat16
F32 = jnp.float32
VLIM = 62 * 1024 * 1024


def gather_blocks(arrays, chunks, order, lsem, rsem, sems):
    nq = len(chunks)
    me = lax.axis_index(AX)
    z, y, x, c = me // 8, lax.rem(me // 4, 2), lax.rem(me // 2, 2), lax.rem(me, 2)

    def dev(z_, y_, x_, c_):
        return ((z_ * 2 + y_) * 2 + x_) * 2 + c_

    d_x, d_y, d_up, d_dn, d_c = dev(z, y, 1 - x, c), dev(z, 1 - y, x, c), me + 8, me - 8, dev(z, y, x, 1 - c)
    bar = pltpu.get_barrier_semaphore()
    for d in (d_x, d_y, d_c):
        pl.semaphore_signal(bar, device_id=(d,), device_id_type=MESH)

    @pl.when(z < 3)
    def _():
        pl.semaphore_signal(bar, device_id=(d_up,), device_id_type=MESH)

    @pl.when(z > 0)
    def _():
        pl.semaphore_signal(bar, device_id=(d_dn,), device_id_type=MESH)

    pl.semaphore_wait(bar, 4 + lax.rem(z + 1, 4) // 2)
    sent = [[[0] for _ in range(4)] for _ in arrays]

    def place(q, zo, yo, xo):
        array, first, rows, _ = chunks[q]
        block, table = arrays[array]
        return table.at[pl.ds(pl.multiple_of(dev(zo, yo, xo, c) * block.shape[0] + first, 8), rows)]

    def slot(q, zo, yo, xo):
        return rsem.at[((zo * 2 + yo) * 2 + xo) * nq + q]

    def forward(q, zo, yo, xo, up, dn, to_x, to_y, src=None):
        dst = place(q, zo, yo, xo)
        src = dst if src is None else src
        ssem, csem = sems[chunks[q][0]]

        def send(d, ss, rs):
            pltpu.make_async_remote_copy(
                src_ref=src, dst_ref=dst, send_sem=ss, recv_sem=rs, device_id=(d,), device_id_type=MESH).start()

        if up is not None:
            @pl.when(up)
            def _():
                send(d_up, ssem.at[0], slot(q, zo, yo, xo))

            @pl.when(dn)
            def _():
                send(d_dn, ssem.at[1], slot(q, zo, yo, xo))
        for there, d, j in ((to_x, d_x, 2), (to_y, d_y, 3)):
            if there:
                send(d, ssem.at[j], slot(q, zo, yo, xo))
                sent[chunks[q][0]][j][0] += chunks[q][2]
        send(d_c, csem.at[0], csem.at[1])

    own = []
    for q in order[:nq]:
        array, first, rows, _ = chunks[q]
        forward(q, z, y, x, z < 3, z > 0, True, True, arrays[array][0].at[pl.ds(first, rows)])
    for j, (block, table) in enumerate(arrays):
        rb = block.shape[0]
        own.append(pltpu.make_async_copy(block, table.at[pl.ds(pl.multiple_of(me * rb, 8), rb)], lsem.at[j]))
        own[j].start()
    zr = [z, z + 1 - 2 * lax.rem(z, 2), 2 - z // 2, 3 - 3 * (z // 2)]

    for code in order[nq:]:
        kind, r, q = code // 100, code // 10 % 10, code % 10
        plane_first = chunks[q][3]
        zo, yo, xo = zr[r], 1 - y if kind >= 2 else y, 1 - x if kind % 2 else x
        here = place(q, zo, yo, xo)
        pltpu.make_async_remote_copy(
            src_ref=here, dst_ref=here, send_sem=sems[0][0].at[0], recv_sem=slot(q, zo, yo, xo),
            device_id=(d_x,), device_id_type=MESH).wait_recv()
        up = dn = None
        if kind == 0 or plane_first:
            up, dn = (z < 3, z > 0) if r == 0 else ((zo < z) & (z < 3), (zo > z) & (z > 0))
        column = kind == 0 and not plane_first
        across = not plane_first or r == 0
        forward(q, zo, yo, xo, up, dn,
                column or (kind == 2 and q % 2 == 1 and across), column or (kind == 1 and q % 2 == 0 and across))

    for j, (block, table) in enumerate(arrays):
        ssem, csem = sems[j]

        def wait_rows(n, sem, table=table):
            v = table.at[pl.ds(0, n)]
            pltpu.make_async_copy(v, v, sem).wait()

        own[j].wait()
        for k in (2, 3):
            wait_rows(sent[j][k][0], ssem.at[k])
        step = sum(rows * (4 if plane_first else 1) for array, _, rows, plane_first in chunks if array == j)
        for k in range(3):
            @pl.when(z == k)
            def _(k=k):
                wait_rows((k + 1) * step, ssem.at[0])

            @pl.when(z == 3 - k)
            def _(k=k):
                wait_rows((k + 1) * step, ssem.at[1])
        wait_rows(16 * block.shape[0], csem.at[0])
        wait_rows(16 * block.shape[0], csem.at[1])


def cut(*sizes, array=0, plane_first=0):
    return [(array, sum(sizes[:i]), n, i < plane_first) for i, n in enumerate(sizes)]


def steps(*words):
    every = [w // 1000 ** i % 1000 for w in words for i in reversed(range(8))]
    return [v for v in every if v != 999]


ROW_CHUNKS = cut(224, 224, 272, 272, 272, 272, 256, 256, plane_first=2)
ROW_ORDER = steps(
    2003006005000004001007, 14100013201206200204016, 12017027023207101116026, 25015036111032033034211,
    24035021213020115215106, 300110022037220125126205, 104225320113112316120136, 224102217130310203011124,
    301227234114235105132237, 135307313212122010236117, 31134210107123216315121, 202223131103127306321311,
    304030317233133222312232, 137221231326331226230302, 303214305330336332322333, 323337325335314327334324)
PACKED_CHUNKS = cut(112, 112, 144, 144, 128, 128, 128, 128, plane_first=2) + cut(168, array=1)
PACKED_ORDER = list(range(9)) + [
    kind * 100 + (s + step) * 10 + q for s in range(5) for q in range(9)
    for kind, step in ((0, 1), (1, 0), (2, 0), (3, -1)) if 0 <= s + step <= 3]


def all_gather(blocks, chunks, order, cid):
    n = len(blocks)

    def kernel(*refs):
        lsem, rsem, *sems = refs[2 * n:]
        gather_blocks(list(zip(refs[:n], refs[n:2 * n])), chunks, order, lsem, rsem, list(zip(sems[::2], sems[1::2])))

    dma = pltpu.SemaphoreType.DMA
    return pl.pallas_call(
        kernel, out_shape=[jax.ShapeDtypeStruct((v.shape[0] * NDEV,) + v.shape[1:], v.dtype) for v in blocks],
        in_specs=[pl.BlockSpec(memory_space=VMEM)] * n, out_specs=[pl.BlockSpec(memory_space=pl.ANY)] * n,
        scratch_shapes=[dma((n,)), dma((16 * len(chunks),))] + [dma((4,)), dma((2,))] * n,
        compiler_params=pltpu.CompilerParams(collective_id=cid, has_side_effects=True))(*blocks)


def gather_rows(v):
    return all_gather([v], ROW_CHUNKS, ROW_ORDER, 2)[0]


def dot(a, b):
    return jnp.dot(a, b, preferred_element_type=F32)


def dot_rows(a, b):
    return lax.dot_general(a, b, (((0,), (0,)), ((), ())), preferred_element_type=F32)


def dot_t(a, b):
    return lax.dot_general(a, b, (((1,), (1,)), ((), ())), preferred_element_type=F32)


CB = 256


def load_table(sources, make, meanwhile=None):
    slots = sources[0][1].shape[0]

    def copies(i, slot):
        for table, space, sem in sources:
            n = space.shape[1]
            rows = table.at[pl.ds(pl.multiple_of(i * n, n), n), :]
            yield pltpu.make_async_copy(rows, space.at[slot], sem.at[slot])

    for i in range(slots - 1):
        for copy in copies(i, i):
            copy.start()
    if meanwhile is not None:
        meanwhile()

    def step(i, _):
        slot = lax.rem(i, slots)
        for copy in copies(i, slot):
            copy.wait()

        @pl.when(i + slots - 1 < NDEV)
        def _():
            for copy in copies(i + slots - 1, lax.rem(i + slots - 1, slots)):
                copy.start()

        make(i, slot)
        return 0

    lax.fori_loop(0, NDEV, step, 0)


def table_mean(tab_hbm, idx_ref, tab, stg, acc, tsem):
    def widen(i, slot):
        tab[pl.ds(pl.multiple_of(i * R, R), R), :] = stg[slot].astype(F32)

    load_table([(tab_hbm, stg, tsem)], widen)
    tab[pl.ds(N, 8), :] = jnp.zeros((8, D), F32)
    slots = [idx_ref.at[pl.ds(k * R, R)] for k in range(K)]

    def body(b, _):
        for u in range(UNROLL):
            r = b * UNROLL + u
            v = [tab[pl.ds(ids[r], 1), :] for ids in slots]
            while len(v) > 1:
                v = [v[j] + v[j + 1] if j + 1 < len(v) else v[j] for j in range(0, len(v), 2)]
            acc[pl.ds(r, 1), :] = v[0]
        return 0

    lax.fori_loop(0, R // UNROLL, body, 0)


TABLE = [VMEM((N + 8, D), F32), VMEM((TBUF, R, D), BF), VMEM((R, D), F32), pltpu.SemaphoreType.DMA((TBUF,))]


def hidden_layer(v, idx, side, w_self, w_nbr):
    def kernel(idx_ref, tab_hbm, x_ref, side_ref, ws_ref, wn_ref, agg_ref, pre_ref, act_ref, tab, stg, acc, tsem):
        table_mean(tab_hbm, idx_ref, tab, stg, acc, tsem)

        def block(i, _):
            r = pl.ds(pl.multiple_of(i * CB, CB), CB)
            agg = (acc[r, :] / side_ref[r, :1]).astype(BF)
            agg_ref[r, :] = agg
            pre = dot(x_ref[r, :], ws_ref[...]) + dot(agg, wn_ref[...])
            pre_ref[r, :] = pre
            act_ref[r, :] = jnp.maximum(pre, 0.0).astype(BF)
            return 0

        lax.fori_loop(0, R // CB, block, 0)

    vm = pl.BlockSpec(memory_space=VMEM)
    return pl.pallas_call(
        kernel,
        out_shape=[jax.ShapeDtypeStruct((R, D), BF), jax.ShapeDtypeStruct((R, D), F32), jax.ShapeDtypeStruct((R, D), BF)],
        in_specs=[pl.BlockSpec(memory_space=pltpu.SMEM), pl.BlockSpec(memory_space=pl.ANY), vm, vm, vm, vm],
        out_specs=[vm] * 3, scratch_shapes=TABLE, compiler_params=pltpu.CompilerParams(vmem_limit_bytes=VLIM),
    )(idx, gather_rows(v), v, side, w_self, w_nbr)


HALF = R // 2


def output_layer(v, idx, side, w_self, w_nbr):
    def kernel(idx_ref, tab_hbm, x_ref, side_ref, ws_ref, wn_ref, g_ref, dws_ref, dwn_ref, loss_ref,
               tab, stg, acc, tsem):
        table_mean(tab_hbm, idx_ref, tab, stg, acc, tsem)
        dws_ref[...] = jnp.zeros((D, D), F32)
        dwn_ref[...] = jnp.zeros((D, D), F32)
        lane = lax.broadcasted_iota(jnp.int32, (CB, D), 1)

        def part(start, half):
            r = pl.ds(pl.multiple_of(start, CB), CB)
            act = x_ref[r, :]
            agg = (acc[r, :] / side_ref[r, :1]).astype(BF)
            logits = dot(act, ws_ref[half]) + dot(agg, wn_ref[half])
            col = lane - half * (D // 2)
            live = (col >= 0) & (col < C)
            top = jnp.max(jnp.where(live, logits, -jnp.inf), axis=1, keepdims=True)
            ex = jnp.where(live, jnp.exp(logits - top), 0.0)
            norm = top + jnp.log(jnp.sum(ex, axis=1, keepdims=True))
            hot = jnp.where(col.astype(F32) == side_ref[r, 1:], 1.0, 0.0)
            loss = jnp.sum(jnp.where(live, hot * (norm - logits), 0.0))
            prob = jnp.where(live, jnp.exp(logits - norm), 0.0)
            g = ((prob - hot) / N).astype(BF)
            dws_ref[...] += dot_rows(act, g)
            dwn_ref[...] += dot_rows(agg, g)
            rest = 1.0 / side_ref[r, :1]
            for j in range(3):
                most = rest.astype(BF)
                g = jnp.where(col == C + j, most, g)
                rest = rest - most.astype(F32)
            return g, loss

        def block(i, loss):
            g_low, loss_low = part(i * CB, 0)
            g_high, loss_high = part(i * CB + HALF, 1)
            g_ref[pl.ds(pl.multiple_of(i * CB, CB), CB), :] = jnp.where(lane < D // 2, g_low, g_high)
            return loss + loss_low + loss_high

        loss = lax.fori_loop(0, HALF // CB, block, jnp.float32(0.0))
        loss_ref[...] = jnp.full((8, D), loss, F32)

    vm = pl.BlockSpec(memory_space=VMEM)
    return pl.pallas_call(
        kernel,
        out_shape=[jax.ShapeDtypeStruct((HALF, D), BF), jax.ShapeDtypeStruct((D, D), F32),
                   jax.ShapeDtypeStruct((D, D), F32), jax.ShapeDtypeStruct((8, D), F32)],
        in_specs=[pl.BlockSpec(memory_space=pltpu.SMEM), pl.BlockSpec(memory_space=pl.ANY)] + [vm] * 4,
        out_specs=[vm] * 4, scratch_shapes=TABLE, compiler_params=pltpu.CompilerParams(vmem_limit_bytes=VLIM),
    )(idx, gather_rows(v), v, side, w_self, w_nbr)


def table_mean_t(lo_ref, hi_ref, lists_hbm, lists, lsem, tab, accs, load):
    def list_copies(s, part, slot):
        off = pl.multiple_of(s * SPAN + (lo_ref[s] // 1024) * 1024 + part * CAP, 1024)
        return [pltpu.make_async_copy(h.at[pl.ds(off, CAP)], b.at[pl.ds(pl.multiple_of(slot * CAP, CAP), CAP)], lsem.at[j, slot])
                for j, (h, b) in enumerate(zip(lists_hbm, lists))]

    for s in range(SLOTS - 1):
        for cp in list_copies(s, 0, s):
            cp.start()

    def clear():
        for a in accs:
            a[...] = jnp.zeros(a.shape, F32)

    load(clear)
    src, dst = [[v.at[pl.ds(u, SLOTS * CAP - EDGES)] for u in range(EDGES)] for v in lists]

    def run(slot, first, last):
        def body(b, _):
            e = slot * CAP + b * EDGES
            for u in range(EDGES):
                d = pl.ds(dst[u][e], 1)
                accs[u % NACC][d, :] += tab[pl.ds(src[u][e], 1), :]
            return 0

        lax.fori_loop(first // EDGES, (last + EDGES - 1) // EDGES, body, 0)

    def sender(s, _):
        slot = lax.rem(s, SLOTS)
        for cp in list_copies(s, 0, slot):
            cp.wait()

        @pl.when(s + SLOTS - 1 < NDEV)
        def _():
            for cp in list_copies(s + SLOTS - 1, 0, lax.rem(s + SLOTS - 1, SLOTS)):
                cp.start()

        base = (lo_ref[s] // 1024) * 1024
        run(slot, lo_ref[s] - base, jnp.minimum(hi_ref[s] - base, CAP))

        def more(p, _):
            for cp in list_copies(s, p, slot):
                cp.start()
            for cp in list_copies(s, p, slot):
                cp.wait()
            run(slot, 0, jnp.minimum(hi_ref[s] - base - p * CAP, CAP))
            return 0

        lax.fori_loop(1, (hi_ref[s] - base + CAP - 1) // CAP, more, 0)
        return 0

    lax.fori_loop(0, NDEV, sender, 0)


def backward_layer(packed, table, lo, hi, lists, g_up, w_self, pre, act, agg, w_nbr, w_up):
    last = table is not None

    def kernel(lo_ref, hi_ref, src_hbm, dst_hbm, packed_hbm, gu_ref, ws_ref, pre_ref, act_ref, agg_ref, *rest):
        if last:
            table_hbm, dws_ref, dwn_ref = rest[:3]
            rest = rest[3:]
        else:
            wn_ref, wu_ref, g_ref, u_ref, dws_ref, dwn_ref = rest[:6]
            rest = rest[6:]
        accs, rest = rest[:NACC], rest[NACC:]
        src, dst, lsem, tab, spread, pstg, psem, *rest = rest

        part_row = lax.broadcasted_iota(jnp.int32, (D, 2 * D), 0) - C
        part_row -= jnp.where(lax.broadcasted_iota(jnp.int32, (D, 2 * D), 1) < D, 0, D // 2)
        spread[...] = jnp.where((part_row >= 0) & (part_row < 3), 1.0, 0.0).astype(BF)

        def make(i, slot):
            for q in range(HALF // CB):
                part = pstg[slot, q * CB:(q + 1) * CB, :]
                scale = dot(part, spread[...])
                if not last:
                    v = dot(part, wu_ref[...]).astype(BF)
                for half in range(2):
                    at = half * HALF + q * CB
                    lanes = slice(half * D, (half + 1) * D)
                    term = rest[0][slot, at:at + CB, :] if last else v[:, lanes]
                    tab[pl.ds(pl.multiple_of(i * R + at, CB), CB), :] = term.astype(F32) * scale[:, lanes]

        sources = [(packed_hbm, pstg, psem)] + ([(table_hbm, *rest)] if last else [])
        table_mean_t(lo_ref, hi_ref, (src_hbm, dst_hbm), (src, dst), lsem, tab, accs,
                     lambda clear: load_table(sources, make, clear))
        dws_ref[...] = jnp.zeros((D, D), F32)
        dwn_ref[...] = jnp.zeros((D, D), F32)

        def part(start, up):
            r = pl.ds(pl.multiple_of(start, CB), CB)
            back = [a[r, :] for a in accs]
            while len(back) > 1:
                back = [back[j] + back[j + 1] for j in range(0, len(back), 2)]
            g = jnp.where(pre_ref[r, :] > 0, up + back[0], 0.0).astype(BF)
            dws_ref[...] += dot_rows(act_ref[r, :], g)
            dwn_ref[...] += dot_rows(agg_ref[r, :], g)
            if not last:
                g_ref[r, :] = g
                u_ref[r, :] = dot_t(g, wn_ref[...]).astype(BF)

        def block(i, _):
            if last:
                part(i * CB, dot_t(gu_ref[pl.ds(pl.multiple_of(i * CB, CB), CB), :], ws_ref[...]))
            else:
                gu = gu_ref[pl.ds(pl.multiple_of(i * CB, CB), CB), :]
                part(i * CB, dot_t(gu, ws_ref[0]))
                part(i * CB + HALF, dot_t(gu, ws_ref[1]))
            return 0

        lax.fori_loop(0, (R if last else HALF) // CB, block, 0)

    vm, sm, hb = (pl.BlockSpec(memory_space=m) for m in (VMEM, pltpu.SMEM, pl.ANY))
    outs = [jax.ShapeDtypeStruct((D, D), F32)] * 2
    args = [lo, hi, *lists, packed, g_up, w_self, pre, act, agg]
    specs = [sm, sm, hb, hb, hb, vm, vm, vm, vm, vm]
    stage = [VMEM((BBUF, HALF, D), BF), pltpu.SemaphoreType.DMA((BBUF,))]
    if last:
        args.append(table)
        specs.append(hb)
        stage += [VMEM((BBUF, R, D), BF), pltpu.SemaphoreType.DMA((BBUF,))]
    else:
        outs = [jax.ShapeDtypeStruct((R, D), BF)] * 2 + outs
        args += [w_nbr, w_up]
        specs += [vm, vm]
    return pl.pallas_call(
        kernel, out_shape=outs, in_specs=specs, out_specs=[vm] * len(outs),
        scratch_shapes=[VMEM((R + 8, D), F32)] * NACC + [pltpu.SMEM((SLOTS * CAP,), jnp.int32)] * 2
        + [pltpu.SemaphoreType.DMA((2, SLOTS)), VMEM((N, D), F32), VMEM((D, 2 * D), BF)] + stage,
        compiler_params=pltpu.CompilerParams(vmem_limit_bytes=VLIM))(*args)


def rank(j):
    return ((j >> 7) & (NDEV - 1)) * R + (j >> 12) * 128 + (j & 127)


SPAN = 21 * 1024


def sorted_edges(ids, live):
    here = jnp.arange(R, dtype=jnp.int32)[None, :]
    key = jnp.where(live, ids * R + here, -1)
    key = lax.sort(key.reshape(E))
    bounds = jnp.arange(NDEV + 1, dtype=jnp.int32)
    starts = jnp.sum(((key >> 22)[None, :] < bounds[:, None]).astype(jnp.int32), axis=1)
    return jnp.concatenate([key.reshape(E // D, D), jnp.pad(starts[None, :], ((0, 7), (0, D - NDEV - 1)))])


def in_edges(every):
    me = lax.axis_index(AX)
    keys = every.reshape(NDEV, SPAN // D, D)
    sender = jnp.arange(NDEV, dtype=jnp.int32)[:, None, None]
    src = rank(sender * R + (keys & (R - 1)))
    dst = (keys >> 11) - me * R
    real = (dst >= 0) & (dst < R) & (keys >= 0) & (jnp.arange(SPAN // D)[None, :, None] < E // D)
    dst = jnp.where(real, dst, R)
    marks = keys[:, E // D, :NDEV + 1]
    lo = lax.dynamic_index_in_dim(marks, me, 1, keepdims=False)
    hi = lax.dynamic_index_in_dim(marks, me + 1, 1, keepdims=False)
    return lo, hi, (src.reshape(-1), dst.reshape(-1))


RED = 24


def reduce_shares(grads, loss, cid):
    n = len(grads)
    step = D // NDEV

    def kernel(*refs):
        loss_ref, own_ref, all_ref, p_ref, got, mine, rsem, ssem, lsem = refs[n:]
        for d in range(NDEV):
            for j in range(n):
                p_ref[d, j * step:(j + 1) * step, :] = refs[j][d * step:(d + 1) * step, :]
            p_ref[d, n * step:, :] = loss_ref[:step, :]
        me = lax.axis_index(AX)
        bar = pltpu.get_barrier_semaphore()

        def greet(k, _):
            pl.semaphore_signal(bar, device_id=(lax.rem(me + k, NDEV),), device_id_type=MESH)
            return 0

        lax.fori_loop(1, NDEV, greet, 0)
        pl.semaphore_wait(bar, NDEV - 1)

        def share(k, _):
            d = lax.rem(me + k, NDEV)
            pltpu.make_async_remote_copy(
                src_ref=p_ref.at[d], dst_ref=got.at[me], send_sem=ssem.at[0], recv_sem=rsem.at[0],
                device_id=(d,), device_id_type=MESH).start()
            return 0

        lax.fori_loop(1, NDEV, share, 0)
        own = pltpu.make_async_copy(p_ref.at[me], got.at[me], lsem.at[0])
        own.start()
        own.wait()
        most = got.at[pl.ds(0, NDEV - 1)]
        pltpu.make_async_copy(most, most, rsem.at[0]).wait()
        v = [got[d] for d in range(NDEV)]
        while len(v) > 1:
            v = [v[j] + v[j + 1] for j in range(0, len(v), 2)]
        own_ref[...] = v[0][:8]
        mine[...] = v[0][8:]

        def tell(k, _):
            d = lax.rem(me + k, NDEV)
            pltpu.make_async_remote_copy(
                src_ref=mine, dst_ref=all_ref.at[me], send_sem=ssem.at[1], recv_sem=rsem.at[1],
                device_id=(d,), device_id_type=MESH).start()
            return 0

        lax.fori_loop(1, NDEV, tell, 0)
        keep = pltpu.make_async_copy(mine, all_ref.at[me], lsem.at[1])
        keep.start()
        keep.wait()
        most = all_ref.at[pl.ds(0, NDEV - 1)]
        pltpu.make_async_copy(most, most, rsem.at[1]).wait()
        pltpu.make_async_copy(most, most, ssem.at[1]).wait()
        most = got.at[pl.ds(0, NDEV - 1)]
        pltpu.make_async_copy(most, most, ssem.at[0]).wait()

    vm = pl.BlockSpec(memory_space=VMEM)
    return pl.pallas_call(
        kernel, name='reduce_shares',
        out_shape=[jax.ShapeDtypeStruct((8, D), F32), jax.ShapeDtypeStruct((NDEV, RED - 8, D), F32)],
        in_specs=[vm] * (n + 1), out_specs=[vm, vm],
        scratch_shapes=[VMEM((NDEV, RED, D), F32)] * 2 + [VMEM((RED - 8, D), F32)] + [pltpu.SemaphoreType.DMA((2,))] * 3,
        compiler_params=pltpu.CompilerParams(collective_id=cid, has_side_effects=True))(*grads, loss)


def solution(mesh):
    def device_step(feat_cols, w_self1_rows, w_nbr1_rows, nbr_rows, mask_rows, w_self2, w_nbr2, w_self3, w_nbr3, label_rows):
        me = lax.axis_index(AX)
        live = mask_rows.T > 0
        ids = rank(nbr_rows.T)
        w1_rows = jnp.concatenate([w_self1_rows, w_nbr1_rows], axis=1)
        out_going = jnp.concatenate(
            [feat_cols.T.reshape(4, 16, NDEV, 128).transpose(2, 0, 1, 3).reshape(NDEV, 4, R),
             jnp.broadcast_to(w1_rows[None], (NDEV, 4, 2 * D))], axis=2)
        in_coming = lax.all_to_all(out_going, AX, 0, 0, tiled=True)
        edges = sorted_edges(ids, live)
        rows = jnp.concatenate([jnp.where(live, ids, N), label_rows[None, :], jnp.zeros((5, R), jnp.int32)])
        blocks = rows.reshape(16, 16, 128).transpose(1, 0, 2)
        blocks = lax.all_to_all(jnp.concatenate([blocks, blocks]), AX, 0, 0, tiled=True)
        rows = lax.dynamic_index_in_dim(blocks.reshape(16, 2, 16, 128), me // 16, 1, keepdims=False)
        rows = rows.transpose(1, 0, 2).reshape(16, R)
        idx, labels = rows[:K], rows[K]
        in_coming = in_coming.reshape(D, R + 2 * D)
        feat = in_coming[:, :R].T
        w_self1, w_nbr1 = in_coming[:, R:R + D], in_coming[:, R + D:]
        deg = jnp.sum((idx < N).astype(F32), axis=0)
        side = jnp.stack([deg, labels.astype(F32)], axis=1)
        idx = idx.reshape(E)
        halves = lambda w: jnp.stack([jnp.pad(w, ((0, 0), (0, D - C))), jnp.pad(w, ((0, 0), (D // 2, D // 2 - C)))])
        ws3, wn3 = halves(w_self3), halves(w_nbr3)
        wn3_t = jnp.concatenate([wn3[0], wn3[1]]).T
        agg_x, pre_one, act_one = hidden_layer(feat, idx, side, w_self1, w_nbr1)
        agg_one, pre_two, act_two = hidden_layer(act_one, idx, side, w_self2, w_nbr2)
        g_three, dws3, dwn3, loss = output_layer(act_two, idx, side, ws3, wn3)
        packed, edges = all_gather([g_three, edges], PACKED_CHUNKS, PACKED_ORDER, 5)
        lo, hi, lists = in_edges(edges)
        g_two, u_one, dws2, dwn2 = backward_layer(
            packed, None, lo, hi, lists, g_three, ws3, pre_two, act_one, agg_one, w_nbr2, wn3_t)
        dws1, dwn1 = backward_layer(
            packed, gather_rows(u_one), lo, hi, lists, g_two, w_self2, pre_one, feat, agg_x, None, None)
        last = jnp.concatenate([v[:, :D // 2] + v[:, D // 2:] for v in (dws3, dwn3)], axis=1)
        own, every = reduce_shares([dws1, dwn1, dws2, dwn2, last], loss, 7)
        whole = lambda j: every[:, j:j + 4].reshape(D, D)
        last = whole(8)
        return (every[0, 12, 0] / N, own[:4], own[4:], whole(0), whole(4), last[:, :C], last[:, D // 2:D // 2 + C])

    row = P(AX, None)
    return jax.shard_map(
        device_step, mesh=mesh,
        in_specs=(P(None, AX), row, row, row, row, P(), P(), P(), P(), P(AX)),
        out_specs=(P(), row, row, P(), P(), P(), P()),
        check_vma=False)
```

```python
import jax
import jax.numpy as jnp
from jax import lax
from jax.experimental import pallas as pl
from jax.experimental.pallas import tpu as pltpu
from jax.sharding import PartitionSpec as P


AX = 'g'
N = 65536
R = 2048
D = 128
K = 10
C = 40
NDEV = 32
E = R * K
CAP = 2048
NACC = 16
EDGES = 32
SLOTS = 8
TBUF = 10
BBUF = 8
UNROLL = 16
MESH = pl.DeviceIdType.MESH
VMEM = pltpu.VMEM
BF = jnp.bfloat16
F32 = jnp.float32
VLIM = 62 * 1024 * 1024
LLIM = 46 * 1024 * 1024
GLIM = 48 * 1024 * 1024


def gather_blocks(arrays, chunks, order, lsem, rsem, sems):
    nq = len(chunks)
    me = lax.axis_index(AX)
    z, y, x, c = me // 8, lax.rem(me // 4, 2), lax.rem(me // 2, 2), lax.rem(me, 2)

    def dev(z_, y_, x_, c_):
        return ((z_ * 2 + y_) * 2 + x_) * 2 + c_

    d_x, d_y, d_up, d_dn, d_c = dev(z, y, 1 - x, c), dev(z, 1 - y, x, c), me + 8, me - 8, dev(z, y, x, 1 - c)
    bar = pltpu.get_barrier_semaphore()
    for d in (d_x, d_y, d_c):
        pl.semaphore_signal(bar, device_id=(d,), device_id_type=MESH)

    @pl.when(z < 3)
    def _():
        pl.semaphore_signal(bar, device_id=(d_up,), device_id_type=MESH)

    @pl.when(z > 0)
    def _():
        pl.semaphore_signal(bar, device_id=(d_dn,), device_id_type=MESH)

    pl.semaphore_wait(bar, 4 + lax.rem(z + 1, 4) // 2)
    sent = [[[0] for _ in range(4)] for _ in arrays]

    def place(q, zo, yo, xo):
        array, first, rows, _ = chunks[q]
        block, table = arrays[array]
        return table.at[pl.ds(pl.multiple_of(dev(zo, yo, xo, c) * block.shape[0] + first, 8), rows)]

    def slot(q, zo, yo, xo):
        return rsem.at[((zo * 2 + yo) * 2 + xo) * nq + q]

    def forward(q, zo, yo, xo, up, dn, to_x, to_y, src=None):
        dst = place(q, zo, yo, xo)
        src = dst if src is None else src
        ssem, csem = sems[chunks[q][0]]

        def send(d, ss, rs):
            pltpu.make_async_remote_copy(
                src_ref=src, dst_ref=dst, send_sem=ss, recv_sem=rs, device_id=(d,), device_id_type=MESH).start()

        if up is not None:
            @pl.when(up)
            def _():
                send(d_up, ssem.at[0], slot(q, zo, yo, xo))

            @pl.when(dn)
            def _():
                send(d_dn, ssem.at[1], slot(q, zo, yo, xo))
        for there, d, j in ((to_x, d_x, 2), (to_y, d_y, 3)):
            if there:
                send(d, ssem.at[j], slot(q, zo, yo, xo))
                sent[chunks[q][0]][j][0] += chunks[q][2]
        send(d_c, csem.at[0], csem.at[1])

    own = []
    for q in order[:nq]:
        array, first, rows, _ = chunks[q]
        forward(q, z, y, x, z < 3, z > 0, True, True, arrays[array][0].at[pl.ds(first, rows)])
    for j, (block, table) in enumerate(arrays):
        rb = block.shape[0]
        own.append(pltpu.make_async_copy(block, table.at[pl.ds(pl.multiple_of(me * rb, 8), rb)], lsem.at[j]))
        own[j].start()
    zr = [z, z + 1 - 2 * lax.rem(z, 2), 2 - z // 2, 3 - 3 * (z // 2)]

    for code in order[nq:]:
        kind, r, q = code // 100, code // 10 % 10, code % 10
        plane_first = chunks[q][3]
        zo, yo, xo = zr[r], 1 - y if kind >= 2 else y, 1 - x if kind % 2 else x
        here = place(q, zo, yo, xo)
        pltpu.make_async_remote_copy(
            src_ref=here, dst_ref=here, send_sem=sems[0][0].at[0], recv_sem=slot(q, zo, yo, xo),
            device_id=(d_x,), device_id_type=MESH).wait_recv()
        up = dn = None
        if kind == 0 or plane_first:
            up, dn = (z < 3, z > 0) if r == 0 else ((zo < z) & (z < 3), (zo > z) & (z > 0))
        column = kind == 0 and not plane_first
        across = not plane_first or r == 0
        forward(q, zo, yo, xo, up, dn,
                column or (kind == 2 and q % 2 == 1 and across), column or (kind == 1 and q % 2 == 0 and across))

    for j, (block, table) in enumerate(arrays):
        ssem, csem = sems[j]

        def wait_rows(n, sem, table=table):
            v = table.at[pl.ds(0, n)]
            pltpu.make_async_copy(v, v, sem).wait()

        own[j].wait()
        for k in (2, 3):
            wait_rows(sent[j][k][0], ssem.at[k])
        step = sum(rows * (4 if plane_first else 1) for array, _, rows, plane_first in chunks if array == j)
        for k in range(3):
            @pl.when(z == k)
            def _(k=k):
                wait_rows((k + 1) * step, ssem.at[0])

            @pl.when(z == 3 - k)
            def _(k=k):
                wait_rows((k + 1) * step, ssem.at[1])
        wait_rows(16 * block.shape[0], csem.at[0])
        wait_rows(16 * block.shape[0], csem.at[1])


def cut(*sizes, array=0, plane_first=0):
    return [(array, sum(sizes[:i]), n, i < plane_first) for i, n in enumerate(sizes)]


def steps(*words):
    every = [w // 1000 ** i % 1000 for w in words for i in reversed(range(8))]
    return [v for v in every if v != 999]


ROW_CHUNKS = cut(224, 224, 272, 272, 272, 272, 256, 256, plane_first=2)
ROW_ORDER = steps(
    2003006005000004001007, 14100013201206200204016, 12017027023207101116026, 25015036111032033034211,
    24035021213020115215106, 300110022037220125126205, 104225320113112316120136, 224102217130310203011124,
    301227234114235105132237, 135307313212122010236117, 31134210107123216315121, 202223131103127306321311,
    304030317233133222312232, 137221231326331226230302, 303214305330336332322333, 323337325335314327334324)
PACKED_CHUNKS = cut(144, 144, 128, 128, 128, 128, 112, 112, plane_first=2) + cut(88, 80, array=1)
PACKED_TURNS = [8, 9, *range(8)]
PACKED_ORDER = PACKED_TURNS + [
    kind * 100 + (s + step) * 10 + q for s in range(5) for q in PACKED_TURNS
    for kind, step in ((0, 1), (1, 0), (2, 0), (3, -1)) if 0 <= s + step <= 3]


def all_gather(blocks, chunks, order, cid, limit):
    n = len(blocks)

    def kernel(*refs):
        lsem, rsem, *sems = refs[2 * n:]
        gather_blocks(list(zip(refs[:n], refs[n:2 * n])), chunks, order, lsem, rsem, list(zip(sems[::2], sems[1::2])))

    dma = pltpu.SemaphoreType.DMA
    return pl.pallas_call(
        kernel, out_shape=[jax.ShapeDtypeStruct((v.shape[0] * NDEV,) + v.shape[1:], v.dtype) for v in blocks],
        in_specs=[pl.BlockSpec(memory_space=VMEM)] * n, out_specs=[pl.BlockSpec(memory_space=pltpu.HBM)] * n,
        scratch_shapes=[dma((n,)), dma((16 * len(chunks),))] + [dma((4,)), dma((2,))] * n,
        compiler_params=pltpu.CompilerParams(
            collective_id=cid, has_side_effects=True, vmem_limit_bytes=limit))(*blocks)


def gather_rows(v):
    return all_gather([v], ROW_CHUNKS, ROW_ORDER, 2, GLIM)[0]


def dot(a, b):
    return jnp.dot(a, b, preferred_element_type=F32)


def dot_rows(a, b):
    return lax.dot_general(a, b, (((0,), (0,)), ((), ())), preferred_element_type=F32)


def dot_t(a, b):
    return lax.dot_general(a, b, (((1,), (1,)), ((), ())), preferred_element_type=F32)


CB = 256


def load_table(sources, make, meanwhile=None):
    slots = sources[0][1].shape[0]

    def copies(i, slot):
        for table, space, sem in sources:
            n = space.shape[1]
            rows = table.at[pl.ds(pl.multiple_of(i * n, n), n), :]
            yield pltpu.make_async_copy(rows, space.at[slot], sem.at[slot])

    for i in range(slots - 1):
        for copy in copies(i, i):
            copy.start()
    if meanwhile is not None:
        meanwhile()

    def step(i, _):
        slot = lax.rem(i, slots)
        for copy in copies(i, slot):
            copy.wait()

        @pl.when(i + slots - 1 < NDEV)
        def _():
            for copy in copies(i + slots - 1, lax.rem(i + slots - 1, slots)):
                copy.start()

        make(i, slot)
        return 0

    lax.fori_loop(0, NDEV, step, 0)


class Inputs:
    def __init__(self, operands, spaces, sem):
        self.copies = [pltpu.make_async_copy(a, b, sem.at[j]) for j, (a, b) in enumerate(zip(operands, spaces))]

    def start(self):
        for copy in self.copies:
            copy.start()


def table_mean(tab_hbm, inputs, idx_ref, tab, stg, acc, tsem):
    def widen(i, slot):
        tab[pl.ds(pl.multiple_of(i * R, R), R), :] = stg[slot].astype(F32)

    load_table([(tab_hbm, stg, tsem)], widen, inputs.start)
    tab[pl.ds(N, 8), :] = jnp.zeros((8, D), F32)
    inputs.copies[0].wait()
    slots = [idx_ref.at[pl.ds(k * R, R)] for k in range(K)]

    def body(b, _):
        for u in range(UNROLL):
            r = b * UNROLL + u
            v = [tab[pl.ds(ids[r], 1), :] for ids in slots]
            while len(v) > 1:
                v = [v[j] + v[j + 1] if j + 1 < len(v) else v[j] for j in range(0, len(v), 2)]
            acc[pl.ds(r, 1), :] = v[0]
        return 0

    lax.fori_loop(0, R // UNROLL, body, 0)
    for copy in inputs.copies[1:]:
        copy.wait()


TABLE = [VMEM((N + 8, D), F32), VMEM((TBUF, R, D), BF), VMEM((R, D), F32), pltpu.SemaphoreType.DMA((TBUF,)),
         pltpu.SMEM((E,), jnp.int32), VMEM((R, D), BF), VMEM((R, 2), F32), pltpu.SemaphoreType.DMA((3,))]
HBM = pl.BlockSpec(memory_space=pltpu.HBM)


def hidden_layer(v, idx, side, w_self, w_nbr):
    def kernel(idx_hbm, tab_hbm, x_hbm, side_hbm, ws_ref, wn_ref, agg_ref, pre_ref, act_ref,
               tab, stg, acc, tsem, idx_ref, x_ref, side_ref, sem):
        inputs = Inputs((idx_hbm, x_hbm, side_hbm), (idx_ref, x_ref, side_ref), sem)
        table_mean(tab_hbm, inputs, idx_ref, tab, stg, acc, tsem)

        def block(i, _):
            r = pl.ds(pl.multiple_of(i * CB, CB), CB)
            agg = (acc[r, :] / side_ref[r, :1]).astype(BF)
            agg_ref[r, :] = agg
            pre = dot(x_ref[r, :], ws_ref[...]) + dot(agg, wn_ref[...])
            pre_ref[r, :] = pre
            act_ref[r, :] = jnp.maximum(pre, 0.0).astype(BF)
            return 0

        lax.fori_loop(0, R // CB, block, 0)

    vm = pl.BlockSpec(memory_space=VMEM)
    return pl.pallas_call(
        kernel,
        out_shape=[jax.ShapeDtypeStruct((R, D), BF), jax.ShapeDtypeStruct((R, D), F32), jax.ShapeDtypeStruct((R, D), BF)],
        in_specs=[HBM] * 4 + [vm] * 2,
        out_specs=[vm] * 3, scratch_shapes=TABLE, compiler_params=pltpu.CompilerParams(vmem_limit_bytes=LLIM),
    )(idx, gather_rows(v), v, side, w_self, w_nbr)


HALF = R // 2


def output_layer(v, idx, side, w_self, w_nbr):
    def kernel(idx_hbm, tab_hbm, x_hbm, side_hbm, ws_ref, wn_ref, g_ref, dws_ref, dwn_ref, loss_ref,
               tab, stg, acc, tsem, idx_ref, x_ref, side_ref, sem):
        inputs = Inputs((idx_hbm, x_hbm, side_hbm), (idx_ref, x_ref, side_ref), sem)
        table_mean(tab_hbm, inputs, idx_ref, tab, stg, acc, tsem)
        dws_ref[...] = jnp.zeros((D, D), F32)
        dwn_ref[...] = jnp.zeros((D, D), F32)
        lane = lax.broadcasted_iota(jnp.int32, (CB, D), 1)

        def part(start, half):
            r = pl.ds(pl.multiple_of(start, CB), CB)
            act = x_ref[r, :]
            agg = (acc[r, :] / side_ref[r, :1]).astype(BF)
            logits = dot(act, ws_ref[half]) + dot(agg, wn_ref[half])
            col = lane - half * (D // 2)
            live = (col >= 0) & (col < C)
            top = jnp.max(jnp.where(live, logits, -jnp.inf), axis=1, keepdims=True)
            ex = jnp.where(live, jnp.exp(logits - top), 0.0)
            norm = top + jnp.log(jnp.sum(ex, axis=1, keepdims=True))
            hot = jnp.where(col.astype(F32) == side_ref[r, 1:], 1.0, 0.0)
            loss = jnp.sum(jnp.where(live, hot * (norm - logits), 0.0))
            prob = jnp.where(live, jnp.exp(logits - norm), 0.0)
            g = ((prob - hot) / N).astype(BF)
            dws_ref[...] += dot_rows(act, g)
            dwn_ref[...] += dot_rows(agg, g)
            rest = 1.0 / side_ref[r, :1]
            for j in range(3):
                most = rest.astype(BF)
                g = jnp.where(col == C + j, most, g)
                rest = rest - most.astype(F32)
            return g, loss

        def block(i, loss):
            g_low, loss_low = part(i * CB, 0)
            g_high, loss_high = part(i * CB + HALF, 1)
            g_ref[pl.ds(pl.multiple_of(i * CB, CB), CB), :] = jnp.where(lane < D // 2, g_low, g_high)
            return loss + loss_low + loss_high

        loss = lax.fori_loop(0, HALF // CB, block, jnp.float32(0.0))
        loss_ref[...] = jnp.full((8, D), loss, F32)

    vm = pl.BlockSpec(memory_space=VMEM)
    return pl.pallas_call(
        kernel,
        out_shape=[jax.ShapeDtypeStruct((HALF, D), BF), jax.ShapeDtypeStruct((D, D), F32),
                   jax.ShapeDtypeStruct((D, D), F32), jax.ShapeDtypeStruct((8, D), F32)],
        in_specs=[HBM] * 4 + [vm] * 2,
        out_specs=[vm] * 4, scratch_shapes=TABLE, compiler_params=pltpu.CompilerParams(vmem_limit_bytes=LLIM),
    )(idx, gather_rows(v), v, side, w_self, w_nbr)


def table_mean_t(lo_ref, hi_ref, lists_hbm, lists, lsem, tab, accs, load, inputs):
    def base_of(s):
        return jnp.minimum(lo_ref[s] // 1024, (SPAN - CAP) // 1024) * 1024

    def list_copies(s, part, slot):
        off = pl.multiple_of(s * SPAN + base_of(s) + part * CAP, 1024)
        return [pltpu.make_async_copy(h.at[pl.ds(off, CAP)], b.at[pl.ds(pl.multiple_of(slot * CAP, CAP), CAP)], lsem.at[j, slot])
                for j, (h, b) in enumerate(zip(lists_hbm, lists))]

    for s in range(SLOTS - 1):
        for cp in list_copies(s, 0, s):
            cp.start()

    def clear():
        inputs.start()
        for a in accs:
            a[...] = jnp.zeros(a.shape, F32)

    load(clear)
    src, dst = [[v.at[pl.ds(u, SLOTS * CAP - EDGES + 1)] for u in range(EDGES)] for v in lists]

    def run(slot, first, last):
        def body(b, _):
            e = slot * CAP + b * EDGES
            for u in range(EDGES):
                d = pl.ds(dst[u][e], 1)
                accs[u % NACC][d, :] += tab[pl.ds(src[u][e], 1), :]
            return 0

        lax.fori_loop(first // EDGES, (last + EDGES - 1) // EDGES, body, 0)

    def sender(s, _):
        slot = lax.rem(s, SLOTS)
        for cp in list_copies(s, 0, slot):
            cp.wait()

        @pl.when(s + SLOTS - 1 < NDEV)
        def _():
            for cp in list_copies(s + SLOTS - 1, 0, lax.rem(s + SLOTS - 1, SLOTS)):
                cp.start()

        base = base_of(s)
        run(slot, lo_ref[s] - base, jnp.minimum(hi_ref[s] - base, CAP))

        def more(p, _):
            for cp in list_copies(s, p, slot):
                cp.start()
            for cp in list_copies(s, p, slot):
                cp.wait()
            run(slot, 0, jnp.minimum(hi_ref[s] - base - p * CAP, CAP))
            return 0

        lax.fori_loop(1, (hi_ref[s] - base + CAP - 1) // CAP, more, 0)
        return 0

    lax.fori_loop(0, NDEV, sender, 0)
    for copy in inputs.copies:
        copy.wait()


def backward_layer(packed, table, lo, hi, lists, g_up, w_self, pre, act, agg, w_nbr, w_up):
    last = table is not None

    def kernel(lo_ref, hi_ref, src_hbm, dst_hbm, packed_hbm, gu_hbm, pre_hbm, act_hbm, agg_hbm, ws_ref, *rest):
        if last:
            table_hbm, dws_ref, dwn_ref = rest[:3]
            rest = rest[3:]
        else:
            wn_ref, wu_ref, g_ref, u_ref, dws_ref, dwn_ref = rest[:6]
            rest = rest[6:]
        accs, rest = rest[:NACC], rest[NACC:]
        src, dst, lsem, tab, spread, gu_ref, pre_ref, act_ref, agg_ref, sem, pstg, psem, *rest = rest
        inputs = Inputs((gu_hbm, pre_hbm, act_hbm, agg_hbm), (gu_ref, pre_ref, act_ref, agg_ref), sem)

        part_row = lax.broadcasted_iota(jnp.int32, (D, 2 * D), 0) - C
        part_row -= jnp.where(lax.broadcasted_iota(jnp.int32, (D, 2 * D), 1) < D, 0, D // 2)
        spread[...] = jnp.where((part_row >= 0) & (part_row < 3), 1.0, 0.0).astype(BF)

        def make(i, slot):
            for q in range(HALF // CB):
                part = pstg[slot, q * CB:(q + 1) * CB, :]
                scale = dot(part, spread[...])
                if not last:
                    v = dot(part, wu_ref[...]).astype(BF)
                for half in range(2):
                    at = half * HALF + q * CB
                    lanes = slice(half * D, (half + 1) * D)
                    term = rest[0][slot, at:at + CB, :] if last else v[:, lanes]
                    tab[pl.ds(pl.multiple_of(i * R + at, CB), CB), :] = term.astype(F32) * scale[:, lanes]

        sources = [(packed_hbm, pstg, psem)] + ([(table_hbm, *rest)] if last else [])
        table_mean_t(lo_ref, hi_ref, (src_hbm, dst_hbm), (src, dst), lsem, tab, accs,
                     lambda clear: load_table(sources, make, clear), inputs)
        dws_ref[...] = jnp.zeros((D, D), F32)
        dwn_ref[...] = jnp.zeros((D, D), F32)

        def part(start, up):
            r = pl.ds(pl.multiple_of(start, CB), CB)
            back = [a[r, :] for a in accs]
            while len(back) > 1:
                back = [back[j] + back[j + 1] for j in range(0, len(back), 2)]
            g = jnp.where(pre_ref[r, :] > 0, up + back[0], 0.0).astype(BF)
            dws_ref[...] += dot_rows(act_ref[r, :], g)
            dwn_ref[...] += dot_rows(agg_ref[r, :], g)
            if not last:
                g_ref[r, :] = g
                u_ref[r, :] = dot_t(g, wn_ref[...]).astype(BF)

        def block(i, _):
            if last:
                part(i * CB, dot_t(gu_ref[pl.ds(pl.multiple_of(i * CB, CB), CB), :], ws_ref[...]))
            else:
                gu = gu_ref[pl.ds(pl.multiple_of(i * CB, CB), CB), :]
                part(i * CB, dot_t(gu, ws_ref[0]))
                part(i * CB + HALF, dot_t(gu, ws_ref[1]))
            return 0

        lax.fori_loop(0, (R if last else HALF) // CB, block, 0)

    vm, sm = (pl.BlockSpec(memory_space=m) for m in (VMEM, pltpu.SMEM))
    outs = [jax.ShapeDtypeStruct((D, D), F32)] * 2
    args = [lo, hi, *lists, packed, g_up, pre, act, agg, w_self]
    specs = [sm, sm] + [HBM] * 7 + [vm]
    stage = [VMEM((BBUF, HALF, D), BF), pltpu.SemaphoreType.DMA((BBUF,))]
    if last:
        args.append(table)
        specs.append(HBM)
        stage += [VMEM((BBUF, R, D), BF), pltpu.SemaphoreType.DMA((BBUF,))]
    else:
        outs = [jax.ShapeDtypeStruct((R, D), BF)] * 2 + outs
        args += [w_nbr, w_up]
        specs += [vm, vm]
    return pl.pallas_call(
        kernel, out_shape=outs, in_specs=specs, out_specs=[vm] * len(outs),
        scratch_shapes=[VMEM((R + 8, D), F32)] * NACC + [pltpu.SMEM((SLOTS * CAP,), jnp.int32)] * 2
        + [pltpu.SemaphoreType.DMA((2, SLOTS)), VMEM((N, D), F32), VMEM((D, 2 * D), BF)]
        + [VMEM(v.shape, v.dtype) for v in (g_up, pre, act, agg)] + [pltpu.SemaphoreType.DMA((4,))] + stage,
        compiler_params=pltpu.CompilerParams(vmem_limit_bytes=VLIM))(*args)


def rank(j):
    return ((j >> 7) & (NDEV - 1)) * R + (j >> 12) * 128 + (j & 127)


SPAN = 21 * 1024


def sorted_edges(ids, live):
    here = jnp.arange(R, dtype=jnp.int32)[None, :]
    key = jnp.where(live, ids * R + here, -1)
    key = lax.sort(key.reshape(E))
    bounds = jnp.arange(NDEV + 1, dtype=jnp.int32)
    starts = jnp.sum(((key >> 22)[None, :] < bounds[:, None]).astype(jnp.int32), axis=1)
    return jnp.concatenate([key.reshape(E // D, D), jnp.pad(starts[None, :], ((0, 7), (0, D - NDEV - 1)))])


def in_edges(every):
    me = lax.axis_index(AX)
    keys = every.reshape(NDEV, SPAN // D, D)
    sender = jnp.arange(NDEV, dtype=jnp.int32)[:, None, None]
    src = rank(sender * R + (keys & (R - 1)))
    dst = (keys >> 11) - me * R
    real = (dst >= 0) & (dst < R) & (keys >= 0) & (jnp.arange(SPAN // D)[None, :, None] < E // D)
    dst = jnp.where(real, dst, R)
    marks = keys[:, E // D, :NDEV + 1]
    lo = lax.dynamic_index_in_dim(marks, me, 1, keepdims=False)
    hi = lax.dynamic_index_in_dim(marks, me + 1, 1, keepdims=False)
    return lo, hi, (src.reshape(-1), dst.reshape(-1))


RED = 24


def reduce_shares(grads, loss, cid):
    n = len(grads)
    step = D // NDEV

    def kernel(*refs):
        loss_ref, own_ref, all_ref, p_ref, got, mine, rsem, ssem, lsem = refs[n:]
        for d in range(NDEV):
            for j in range(n):
                p_ref[d, j * step:(j + 1) * step, :] = refs[j][d * step:(d + 1) * step, :]
            p_ref[d, n * step:, :] = loss_ref[:step, :]
        me = lax.axis_index(AX)
        bar = pltpu.get_barrier_semaphore()

        def greet(k, _):
            pl.semaphore_signal(bar, device_id=(lax.rem(me + k, NDEV),), device_id_type=MESH)
            return 0

        lax.fori_loop(1, NDEV, greet, 0)
        pl.semaphore_wait(bar, NDEV - 1)

        def share(k, _):
            d = lax.rem(me + k, NDEV)
            pltpu.make_async_remote_copy(
                src_ref=p_ref.at[d], dst_ref=got.at[me], send_sem=ssem.at[0], recv_sem=rsem.at[0],
                device_id=(d,), device_id_type=MESH).start()
            return 0

        lax.fori_loop(1, NDEV, share, 0)
        own = pltpu.make_async_copy(p_ref.at[me], got.at[me], lsem.at[0])
        own.start()
        own.wait()
        most = got.at[pl.ds(0, NDEV - 1)]
        pltpu.make_async_copy(most, most, rsem.at[0]).wait()
        v = [got[d] for d in range(NDEV)]
        while len(v) > 1:
            v = [v[j] + v[j + 1] for j in range(0, len(v), 2)]
        own_ref[...] = v[0][:8]
        mine[...] = v[0][8:]

        def tell(k, _):
            d = lax.rem(me + k, NDEV)
            pltpu.make_async_remote_copy(
                src_ref=mine, dst_ref=all_ref.at[me], send_sem=ssem.at[1], recv_sem=rsem.at[1],
                device_id=(d,), device_id_type=MESH).start()
            return 0

        lax.fori_loop(1, NDEV, tell, 0)
        keep = pltpu.make_async_copy(mine, all_ref.at[me], lsem.at[1])
        keep.start()
        keep.wait()
        most = all_ref.at[pl.ds(0, NDEV - 1)]
        pltpu.make_async_copy(most, most, rsem.at[1]).wait()
        pltpu.make_async_copy(most, most, ssem.at[1]).wait()
        most = got.at[pl.ds(0, NDEV - 1)]
        pltpu.make_async_copy(most, most, ssem.at[0]).wait()

    vm = pl.BlockSpec(memory_space=VMEM)
    return pl.pallas_call(
        kernel, name='reduce_shares',
        out_shape=[jax.ShapeDtypeStruct((8, D), F32), jax.ShapeDtypeStruct((NDEV, RED - 8, D), F32)],
        in_specs=[vm] * (n + 1), out_specs=[vm, vm],
        scratch_shapes=[VMEM((NDEV, RED, D), F32)] * 2 + [VMEM((RED - 8, D), F32)] + [pltpu.SemaphoreType.DMA((2,))] * 3,
        compiler_params=pltpu.CompilerParams(collective_id=cid, has_side_effects=True))(*grads, loss)


def solution(mesh):
    def device_step(feat_cols, w_self1_rows, w_nbr1_rows, nbr_rows, mask_rows, w_self2, w_nbr2, w_self3, w_nbr3, label_rows):
        me = lax.axis_index(AX)
        live = mask_rows.T > 0
        ids = rank(nbr_rows.T)
        w1_rows = jnp.concatenate([w_self1_rows, w_nbr1_rows], axis=1)
        out_going = jnp.concatenate(
            [feat_cols.T.reshape(4, 16, NDEV, 128).transpose(2, 0, 1, 3).reshape(NDEV, 4, R),
             jnp.broadcast_to(w1_rows[None], (NDEV, 4, 2 * D))], axis=2)
        in_coming = lax.all_to_all(out_going, AX, 0, 0, tiled=True)
        edges = sorted_edges(ids, live)
        rows = jnp.concatenate([jnp.where(live, ids, N), label_rows[None, :], jnp.zeros((5, R), jnp.int32)])
        blocks = rows.reshape(16, 16, 128).transpose(1, 0, 2)
        blocks = lax.all_to_all(jnp.concatenate([blocks, blocks]), AX, 0, 0, tiled=True)
        rows = lax.dynamic_index_in_dim(blocks.reshape(16, 2, 16, 128), me // 16, 1, keepdims=False)
        rows = rows.transpose(1, 0, 2).reshape(16, R)
        idx, labels = rows[:K], rows[K]
        in_coming = in_coming.reshape(D, R + 2 * D)
        feat = in_coming[:, :R].T
        w_self1, w_nbr1 = in_coming[:, R:R + D], in_coming[:, R + D:]
        deg = jnp.sum((idx < N).astype(F32), axis=0)
        side = jnp.stack([deg, labels.astype(F32)], axis=1)
        idx = idx.reshape(E)
        halves = lambda w: jnp.stack([jnp.pad(w, ((0, 0), (0, D - C))), jnp.pad(w, ((0, 0), (D // 2, D // 2 - C)))])
        ws3, wn3 = halves(w_self3), halves(w_nbr3)
        wn3_t = jnp.concatenate([wn3[0], wn3[1]]).T
        agg_x, pre_one, act_one = hidden_layer(feat, idx, side, w_self1, w_nbr1)
        agg_one, pre_two, act_two = hidden_layer(act_one, idx, side, w_self2, w_nbr2)
        g_three, dws3, dwn3, loss = output_layer(act_two, idx, side, ws3, wn3)
        packed, edges = all_gather([g_three, edges], PACKED_CHUNKS, PACKED_ORDER, 5, VLIM)
        lo, hi, lists = in_edges(edges)
        g_two, u_one, dws2, dwn2 = backward_layer(
            packed, None, lo, hi, lists, g_three, ws3, pre_two, act_one, agg_one, w_nbr2, wn3_t)
        dws1, dwn1 = backward_layer(
            packed, gather_rows(u_one), lo, hi, lists, g_two, w_self2, pre_one, feat, agg_x, None, None)
        last = jnp.concatenate([v[:, :D // 2] + v[:, D // 2:] for v in (dws3, dwn3)], axis=1)
        own, every = reduce_shares([dws1, dwn1, dws2, dwn2, last], loss, 7)
        whole = lambda j: every[:, j:j + 4].reshape(D, D)
        last = whole(8)
        return (every[0, 12, 0] / N, own[:4], own[4:], whole(0), whole(4), last[:, :C], last[:, D // 2:D // 2 + C])

    row = P(AX, None)
    return jax.shard_map(
        device_step, mesh=mesh,
        in_specs=(P(None, AX), row, row, row, row, P(), P(), P(), P(), P(AX)),
        out_specs=(P(), row, row, P(), P(), P(), P()),
        check_vma=False)
```

```python
import jax
import jax.numpy as jnp
from jax import lax
from jax.experimental import pallas as pl
from jax.experimental.pallas import tpu as pltpu
from jax.sharding import PartitionSpec as P


AX = 'g'
N = 65536
R = 2048
D = 128
K = 10
C = 40
NDEV = 32
E = R * K
CAP = 2048
NACC = 8
EDGES = 64
SLOTS = 8
TBUF = 10
BBUF = 8
UNROLL = 32
MESH = pl.DeviceIdType.MESH
VMEM = pltpu.VMEM
BF = jnp.bfloat16
F32 = jnp.float32
VLIM = 62 * 1024 * 1024
LLIM = 46 * 1024 * 1024
GLIM = 48 * 1024 * 1024


def gather_blocks(arrays, chunks, order, lsem, rsem, sems):
    nq = len(chunks)
    me = lax.axis_index(AX)
    z, y, x, c = me // 8, lax.rem(me // 4, 2), lax.rem(me // 2, 2), lax.rem(me, 2)

    def dev(z_, y_, x_, c_):
        return ((z_ * 2 + y_) * 2 + x_) * 2 + c_

    d_x, d_y, d_up, d_dn, d_c = dev(z, y, 1 - x, c), dev(z, 1 - y, x, c), me + 8, me - 8, dev(z, y, x, 1 - c)
    bar = pltpu.get_barrier_semaphore()
    for d in (d_x, d_y, d_c):
        pl.semaphore_signal(bar, device_id=(d,), device_id_type=MESH)

    @pl.when(z < 3)
    def _():
        pl.semaphore_signal(bar, device_id=(d_up,), device_id_type=MESH)

    @pl.when(z > 0)
    def _():
        pl.semaphore_signal(bar, device_id=(d_dn,), device_id_type=MESH)

    pl.semaphore_wait(bar, 4 + lax.rem(z + 1, 4) // 2)
    sent = [[[0] for _ in range(4)] for _ in arrays]

    def place(q, zo, yo, xo):
        array, first, rows, _ = chunks[q]
        block, table = arrays[array]
        return table.at[pl.ds(pl.multiple_of(dev(zo, yo, xo, c) * block.shape[0] + first, 8), rows)]

    def slot(q, zo, yo, xo):
        return rsem.at[((zo * 2 + yo) * 2 + xo) * nq + q]

    def forward(q, zo, yo, xo, up, dn, to_x, to_y, src=None):
        dst = place(q, zo, yo, xo)
        src = dst if src is None else src
        ssem, csem = sems[chunks[q][0]]

        def send(d, ss, rs):
            pltpu.make_async_remote_copy(
                src_ref=src, dst_ref=dst, send_sem=ss, recv_sem=rs, device_id=(d,), device_id_type=MESH).start()

        if up is not None:
            @pl.when(up)
            def _():
                send(d_up, ssem.at[0], slot(q, zo, yo, xo))

            @pl.when(dn)
            def _():
                send(d_dn, ssem.at[1], slot(q, zo, yo, xo))
        for there, d, j in ((to_x, d_x, 2), (to_y, d_y, 3)):
            if there:
                send(d, ssem.at[j], slot(q, zo, yo, xo))
                sent[chunks[q][0]][j][0] += chunks[q][2]
        send(d_c, csem.at[0], csem.at[1])

    own = []
    for q in order[:nq]:
        array, first, rows, _ = chunks[q]
        forward(q, z, y, x, z < 3, z > 0, True, True, arrays[array][0].at[pl.ds(first, rows)])
    for j, (block, table) in enumerate(arrays):
        rb = block.shape[0]
        own.append(pltpu.make_async_copy(block, table.at[pl.ds(pl.multiple_of(me * rb, 8), rb)], lsem.at[j]))
        own[j].start()
    zr = [z, z + 1 - 2 * lax.rem(z, 2), 2 - z // 2, 3 - 3 * (z // 2)]

    for code in order[nq:]:
        kind, r, q = code // 100, code // 10 % 10, code % 10
        plane_first = chunks[q][3]
        zo, yo, xo = zr[r], 1 - y if kind >= 2 else y, 1 - x if kind % 2 else x
        here = place(q, zo, yo, xo)
        pltpu.make_async_remote_copy(
            src_ref=here, dst_ref=here, send_sem=sems[0][0].at[0], recv_sem=slot(q, zo, yo, xo),
            device_id=(d_x,), device_id_type=MESH).wait_recv()
        up = dn = None
        if kind == 0 or plane_first:
            up, dn = (z < 3, z > 0) if r == 0 else ((zo < z) & (z < 3), (zo > z) & (z > 0))
        column = kind == 0 and not plane_first
        across = not plane_first or r == 0
        forward(q, zo, yo, xo, up, dn,
                column or (kind == 2 and q % 2 == 1 and across), column or (kind == 1 and q % 2 == 0 and across))

    for j, (block, table) in enumerate(arrays):
        ssem, csem = sems[j]

        def wait_rows(n, sem, table=table):
            v = table.at[pl.ds(0, n)]
            pltpu.make_async_copy(v, v, sem).wait()

        own[j].wait()
        for k in (2, 3):
            wait_rows(sent[j][k][0], ssem.at[k])
        step = sum(rows * (4 if plane_first else 1) for array, _, rows, plane_first in chunks if array == j)
        for k in range(3):
            @pl.when(z == k)
            def _(k=k):
                wait_rows((k + 1) * step, ssem.at[0])

            @pl.when(z == 3 - k)
            def _(k=k):
                wait_rows((k + 1) * step, ssem.at[1])
        wait_rows(16 * block.shape[0], csem.at[0])
        wait_rows(16 * block.shape[0], csem.at[1])


def cut(*sizes, array=0, plane_first=0):
    return [(array, sum(sizes[:i]), n, i < plane_first) for i, n in enumerate(sizes)]


def steps(*words):
    every = [w // 1000 ** i % 1000 for w in words for i in reversed(range(8))]
    return [v for v in every if v != 999]


ROW_CHUNKS = cut(224, 224, 272, 272, 272, 272, 256, 256, plane_first=2)
ROW_ORDER = steps(
    2003006005000004001007, 14100013201206200204016, 12017027023207101116026, 25015036111032033034211,
    24035021213020115215106, 300110022037220125126205, 104225320113112316120136, 224102217130310203011124,
    301227234114235105132237, 135307313212122010236117, 31134210107123216315121, 202223131103127306321311,
    304030317233133222312232, 137221231326331226230302, 303214305330336332322333, 323337325335314327334324)
PACKED_CHUNKS = cut(144, 144, 128, 128, 128, 128, 112, 112, plane_first=2) + cut(88, 80, array=1)
PACKED_TURNS = [8, 9, *range(8)]
PACKED_ORDER = PACKED_TURNS + [
    kind * 100 + (s + step) * 10 + q for s in range(5) for q in PACKED_TURNS
    for kind, step in ((0, 1), (1, 0), (2, 0), (3, -1)) if 0 <= s + step <= 3]


def all_gather(blocks, chunks, order, cid, limit):
    n = len(blocks)

    def kernel(*refs):
        lsem, rsem, *sems = refs[2 * n:]
        gather_blocks(list(zip(refs[:n], refs[n:2 * n])), chunks, order, lsem, rsem, list(zip(sems[::2], sems[1::2])))

    dma = pltpu.SemaphoreType.DMA
    return pl.pallas_call(
        kernel, out_shape=[jax.ShapeDtypeStruct((v.shape[0] * NDEV,) + v.shape[1:], v.dtype) for v in blocks],
        in_specs=[pl.BlockSpec(memory_space=VMEM)] * n, out_specs=[pl.BlockSpec(memory_space=pltpu.HBM)] * n,
        scratch_shapes=[dma((n,)), dma((16 * len(chunks),))] + [dma((4,)), dma((2,))] * n,
        compiler_params=pltpu.CompilerParams(
            collective_id=cid, has_side_effects=True, vmem_limit_bytes=limit))(*blocks)


def gather_rows(v):
    return all_gather([v], ROW_CHUNKS, ROW_ORDER, 2, GLIM)[0]


def dot(a, b):
    return jnp.dot(a, b, preferred_element_type=F32)


def dot_rows(a, b):
    return lax.dot_general(a, b, (((0,), (0,)), ((), ())), preferred_element_type=F32)


def dot_t(a, b):
    return lax.dot_general(a, b, (((1,), (1,)), ((), ())), preferred_element_type=F32)


CB = 256


def load_table(sources, make, meanwhile=None):
    slots = sources[0][1].shape[0]

    def copies(i, slot):
        for table, space, sem in sources:
            n = space.shape[1]
            rows = table.at[pl.ds(pl.multiple_of(i * n, n), n), :]
            yield pltpu.make_async_copy(rows, space.at[slot], sem.at[slot])

    for i in range(slots - 1):
        for copy in copies(i, i):
            copy.start()
    if meanwhile is not None:
        meanwhile()

    def step(i, _):
        slot = lax.rem(i, slots)
        for copy in copies(i, slot):
            copy.wait()

        @pl.when(i + slots - 1 < NDEV)
        def _():
            for copy in copies(i + slots - 1, lax.rem(i + slots - 1, slots)):
                copy.start()

        make(i, slot)
        return 0

    lax.fori_loop(0, NDEV, step, 0)


class Inputs:
    def __init__(self, operands, spaces, sem):
        self.copies = [pltpu.make_async_copy(a, b, sem.at[j]) for j, (a, b) in enumerate(zip(operands, spaces))]

    def start(self):
        for copy in self.copies:
            copy.start()


def table_mean(tab_hbm, inputs, idx_ref, tab, stg, acc, tsem):
    def widen(i, slot):
        tab[pl.ds(pl.multiple_of(i * R, R), R), :] = stg[slot].astype(F32)

    load_table([(tab_hbm, stg, tsem)], widen, inputs.start)
    tab[pl.ds(N, 8), :] = jnp.zeros((8, D), F32)
    inputs.copies[0].wait()
    slots = [idx_ref.at[pl.ds(k * R, R)] for k in range(K)]

    def body(b, _):
        for u in range(UNROLL):
            r = b * UNROLL + u
            acc[pl.ds(r, 1), :] = total([tab[pl.ds(ids[r], 1), :] for ids in slots])
        return 0

    lax.fori_loop(0, R // UNROLL, body, 0)
    for copy in inputs.copies[1:]:
        copy.wait()


TABLE = [VMEM((N + 8, D), F32), VMEM((TBUF, R, D), BF), VMEM((R, D), F32), pltpu.SemaphoreType.DMA((TBUF,)),
         pltpu.SMEM((E,), jnp.int32), VMEM((R, D), BF), VMEM((R, 2), F32), pltpu.SemaphoreType.DMA((3,))]
HBM = pl.BlockSpec(memory_space=pltpu.HBM)


def hidden_layer(v, idx, side, w_self, w_nbr):
    def kernel(idx_hbm, tab_hbm, x_hbm, side_hbm, ws_ref, wn_ref, agg_ref, pre_ref, act_ref,
               tab, stg, acc, tsem, idx_ref, x_ref, side_ref, sem):
        inputs = Inputs((idx_hbm, x_hbm, side_hbm), (idx_ref, x_ref, side_ref), sem)
        table_mean(tab_hbm, inputs, idx_ref, tab, stg, acc, tsem)

        def block(i, _):
            r = pl.ds(pl.multiple_of(i * CB, CB), CB)
            agg = (acc[r, :] / side_ref[r, :1]).astype(BF)
            agg_ref[r, :] = agg
            pre = dot(x_ref[r, :], ws_ref[...]) + dot(agg, wn_ref[...])
            pre_ref[r, :] = pre
            act_ref[r, :] = jnp.maximum(pre, 0.0).astype(BF)
            return 0

        lax.fori_loop(0, R // CB, block, 0)

    vm = pl.BlockSpec(memory_space=VMEM)
    return pl.pallas_call(
        kernel,
        out_shape=[jax.ShapeDtypeStruct((R, D), BF), jax.ShapeDtypeStruct((R, D), F32), jax.ShapeDtypeStruct((R, D), BF)],
        in_specs=[HBM] * 4 + [vm] * 2,
        out_specs=[vm] * 3, scratch_shapes=TABLE, compiler_params=pltpu.CompilerParams(vmem_limit_bytes=LLIM),
    )(idx, gather_rows(v), v, side, w_self, w_nbr)


HALF = R // 2


def output_layer(v, idx, side, w_self, w_nbr):
    def kernel(idx_hbm, tab_hbm, x_hbm, side_hbm, ws_ref, wn_ref, g_ref, dws_ref, dwn_ref, loss_ref,
               tab, stg, acc, tsem, idx_ref, x_ref, side_ref, sem):
        inputs = Inputs((idx_hbm, x_hbm, side_hbm), (idx_ref, x_ref, side_ref), sem)
        table_mean(tab_hbm, inputs, idx_ref, tab, stg, acc, tsem)
        dws_ref[...] = jnp.zeros((D, D), F32)
        dwn_ref[...] = jnp.zeros((D, D), F32)
        lane = lax.broadcasted_iota(jnp.int32, (CB, D), 1)

        def part(start, half):
            r = pl.ds(pl.multiple_of(start, CB), CB)
            act = x_ref[r, :]
            agg = (acc[r, :] / side_ref[r, :1]).astype(BF)
            logits = dot(act, ws_ref[half]) + dot(agg, wn_ref[half])
            col = lane - half * (D // 2)
            live = (col >= 0) & (col < C)
            top = jnp.max(jnp.where(live, logits, -jnp.inf), axis=1, keepdims=True)
            ex = jnp.where(live, jnp.exp(logits - top), 0.0)
            norm = top + jnp.log(jnp.sum(ex, axis=1, keepdims=True))
            hot = jnp.where(col.astype(F32) == side_ref[r, 1:], 1.0, 0.0)
            loss = jnp.sum(jnp.where(live, hot * (norm - logits), 0.0))
            prob = jnp.where(live, jnp.exp(logits - norm), 0.0)
            g = ((prob - hot) / N).astype(BF)
            dws_ref[...] += dot_rows(act, g)
            dwn_ref[...] += dot_rows(agg, g)
            rest = 1.0 / side_ref[r, :1]
            for j in range(3):
                most = rest.astype(BF)
                g = jnp.where(col == C + j, most, g)
                rest = rest - most.astype(F32)
            return g, loss

        def block(i, loss):
            g_low, loss_low = part(i * CB, 0)
            g_high, loss_high = part(i * CB + HALF, 1)
            g_ref[pl.ds(pl.multiple_of(i * CB, CB), CB), :] = jnp.where(lane < D // 2, g_low, g_high)
            return loss + loss_low + loss_high

        loss = lax.fori_loop(0, HALF // CB, block, jnp.float32(0.0))
        loss_ref[...] = jnp.full((8, D), loss, F32)

    vm = pl.BlockSpec(memory_space=VMEM)
    return pl.pallas_call(
        kernel,
        out_shape=[jax.ShapeDtypeStruct((HALF, D), BF), jax.ShapeDtypeStruct((D, D), F32),
                   jax.ShapeDtypeStruct((D, D), F32), jax.ShapeDtypeStruct((8, D), F32)],
        in_specs=[HBM] * 4 + [vm] * 2,
        out_specs=[vm] * 4, scratch_shapes=TABLE, compiler_params=pltpu.CompilerParams(vmem_limit_bytes=LLIM),
    )(idx, gather_rows(v), v, side, w_self, w_nbr)


def table_mean_t(fetch, marks, lists_hbm, lists, lsem, tab, accs, load, inputs):
    me = lax.axis_index(AX)

    def base_of(s):
        return jnp.minimum(marks[s, me] // 1024, (SPAN - CAP) // 1024) * 1024

    def list_copies(s, part, slot):
        off = pl.multiple_of(s * SPAN + base_of(s) + part * CAP, 1024)
        return [pltpu.make_async_copy(h.at[pl.ds(off, CAP)], b.at[pl.ds(pl.multiple_of(slot * CAP, CAP), CAP)], lsem.at[j, slot])
                for j, (h, b) in enumerate(zip(lists_hbm, lists))]

    def clear():
        inputs.start()
        for a in accs:
            a[...] = jnp.zeros(a.shape, F32)
        fetch.wait()
        for s in range(SLOTS - 1):
            for cp in list_copies(s, 0, s):
                cp.start()

    load(clear)
    src, dst = [[v.at[pl.ds(u, SLOTS * CAP - EDGES + 1)] for u in range(EDGES)] for v in lists]

    def run(slot, first, last):
        def body(b, _):
            e = slot * CAP + b * EDGES
            for u in range(EDGES):
                d = pl.ds(dst[u][e], 1)
                accs[u % NACC][d, :] += tab[pl.ds(src[u][e], 1), :]
            return 0

        lax.fori_loop(first // EDGES, (last + EDGES - 1) // EDGES, body, 0)

    def sender(s, _):
        slot = lax.rem(s, SLOTS)
        for cp in list_copies(s, 0, slot):
            cp.wait()

        @pl.when(s + SLOTS - 1 < NDEV)
        def _():
            for cp in list_copies(s + SLOTS - 1, 0, lax.rem(s + SLOTS - 1, SLOTS)):
                cp.start()

        base = base_of(s)
        end = marks[s, me + 1] - base
        run(slot, marks[s, me] - base, jnp.minimum(end, CAP))

        def more(p, _):
            for cp in list_copies(s, p, slot):
                cp.start()
            for cp in list_copies(s, p, slot):
                cp.wait()
            run(slot, 0, jnp.minimum(end - p * CAP, CAP))
            return 0

        lax.fori_loop(1, (end + CAP - 1) // CAP, more, 0)
        return 0

    lax.fori_loop(0, NDEV, sender, 0)
    for copy in inputs.copies:
        copy.wait()


def backward_layer(packed, table, edges, lists, g_up, w_self, pre, act, agg, w_nbr, w_up):
    last = table is not None

    def kernel(edges_hbm, src_hbm, dst_hbm, packed_hbm, gu_hbm, pre_hbm, act_hbm, agg_hbm, ws_ref, *rest):
        if last:
            table_hbm, dws_ref, dwn_ref = rest[:3]
            rest = rest[3:]
        else:
            wn_ref, wu_ref, g_ref, u_ref, dws_ref, dwn_ref = rest[:6]
            rest = rest[6:]
        accs, rest = rest[:NACC], rest[NACC:]
        marks, src, dst, lsem, tab, spread, gu_ref, pre_ref, act_ref, agg_ref, sem, pstg, psem, *rest = rest
        inputs = Inputs((gu_hbm, pre_hbm, act_hbm, agg_hbm), (gu_ref, pre_ref, act_ref, agg_ref), sem)
        fetch = pltpu.make_async_copy(edges_hbm.at[:, E // D, :], marks, sem.at[4])
        fetch.start()

        part_row = lax.broadcasted_iota(jnp.int32, (D, 2 * D), 0) - C
        part_row -= jnp.where(lax.broadcasted_iota(jnp.int32, (D, 2 * D), 1) < D, 0, D // 2)
        spread[...] = jnp.where((part_row >= 0) & (part_row < 3), 1.0, 0.0).astype(BF)

        def make(i, slot):
            for q in range(HALF // CB):
                part = pstg[slot, q * CB:(q + 1) * CB, :]
                scale = dot(part, spread[...])
                if not last:
                    v = dot(part, wu_ref[...]).astype(BF)
                for half in range(2):
                    at = half * HALF + q * CB
                    lanes = slice(half * D, (half + 1) * D)
                    term = rest[0][slot, at:at + CB, :] if last else v[:, lanes]
                    tab[pl.ds(pl.multiple_of(i * R + at, CB), CB), :] = term.astype(F32) * scale[:, lanes]

        sources = [(packed_hbm, pstg, psem)] + ([(table_hbm, *rest)] if last else [])
        table_mean_t(fetch, marks, (src_hbm, dst_hbm), (src, dst), lsem, tab, accs,
                     lambda clear: load_table(sources, make, clear), inputs)
        dws_ref[...] = jnp.zeros((D, D), F32)
        dwn_ref[...] = jnp.zeros((D, D), F32)

        def part(start, up):
            r = pl.ds(pl.multiple_of(start, CB), CB)
            g = jnp.where(pre_ref[r, :] > 0, up + total([a[r, :] for a in accs]), 0.0).astype(BF)
            dws_ref[...] += dot_rows(act_ref[r, :], g)
            dwn_ref[...] += dot_rows(agg_ref[r, :], g)
            if not last:
                g_ref[r, :] = g
                u_ref[r, :] = dot_t(g, wn_ref[...]).astype(BF)

        def block(i, _):
            if last:
                part(i * CB, dot_t(gu_ref[pl.ds(pl.multiple_of(i * CB, CB), CB), :], ws_ref[...]))
            else:
                gu = gu_ref[pl.ds(pl.multiple_of(i * CB, CB), CB), :]
                part(i * CB, dot_t(gu, ws_ref[0]))
                part(i * CB + HALF, dot_t(gu, ws_ref[1]))
            return 0

        lax.fori_loop(0, (R if last else HALF) // CB, block, 0)

    vm = pl.BlockSpec(memory_space=VMEM)
    outs = [jax.ShapeDtypeStruct((D, D), F32)] * 2
    args = [edges.reshape(NDEV, SPAN // D, D), *lists, packed, g_up, pre, act, agg, w_self]
    specs = [HBM] * 8 + [vm]
    stage = [VMEM((BBUF, HALF, D), BF), pltpu.SemaphoreType.DMA((BBUF,))]
    if last:
        args.append(table)
        specs.append(HBM)
        stage += [VMEM((BBUF, R, D), BF), pltpu.SemaphoreType.DMA((BBUF,))]
    else:
        outs = [jax.ShapeDtypeStruct((R, D), BF)] * 2 + outs
        args += [w_nbr, w_up]
        specs += [vm, vm]
    return pl.pallas_call(
        kernel, out_shape=outs, in_specs=specs, out_specs=[vm] * len(outs),
        scratch_shapes=[VMEM((R + 8, D), F32)] * NACC + [pltpu.SMEM((NDEV, D), jnp.int32)] + [pltpu.SMEM((SLOTS * CAP,), jnp.int32)] * 2
        + [pltpu.SemaphoreType.DMA((2, SLOTS)), VMEM((N, D), F32), VMEM((D, 2 * D), BF)]
        + [VMEM(v.shape, v.dtype) for v in (g_up, pre, act, agg)] + [pltpu.SemaphoreType.DMA((5,))] + stage,
        compiler_params=pltpu.CompilerParams(vmem_limit_bytes=VLIM))(*args)


def rank(j):
    return ((j >> 7) & (NDEV - 1)) * R + (j >> 12) * 128 + (j & 127)


SPAN = 21 * 1024


def sorted_edges(ids, live):
    here = jnp.arange(R, dtype=jnp.int32)[None, :]
    key = jnp.where(live, ids * R + here, -1)
    key = lax.sort(key.reshape(E))
    bounds = jnp.arange(NDEV + 1, dtype=jnp.int32)
    starts = jnp.sum(((key >> 22)[None, :] < bounds[:, None]).astype(jnp.int32), axis=1)
    return jnp.concatenate([key.reshape(E // D, D), jnp.pad(starts[None, :], ((0, 7), (0, D - NDEV - 1)))])


def in_edges(every):
    me = lax.axis_index(AX)
    keys = every.reshape(NDEV, SPAN // D, D)
    sender = jnp.arange(NDEV, dtype=jnp.int32)[:, None, None]
    src = rank(sender * R + (keys & (R - 1)))
    dst = (keys >> 11) - me * R
    real = (dst >= 0) & (dst < R) & (keys >= 0) & (jnp.arange(SPAN // D)[None, :, None] < E // D)
    dst = jnp.where(real, dst, R)
    return src.reshape(-1), dst.reshape(-1)


RED = 24


def total(v):
    while len(v) > 1:
        v = [v[j] + v[j + 1] if j + 1 < len(v) else v[j] for j in range(0, len(v), 2)]
    return v[0]


def reduce_shares(grads, loss, cid):
    n = len(grads)
    step = D // NDEV
    kept, told = pl.ds(0, 2 * step), pl.ds(2 * step, RED - 2 * step)

    def kernel(*refs):
        loss_ref, own_ref, all_ref, p_ref, got, mine, rsem, ssem, lsem = refs[n:]
        for d in range(NDEV):
            for j in range(n):
                p_ref[d, j * step:(j + 1) * step, :] = refs[j][d * step:(d + 1) * step, :]
            p_ref[d, n * step:, :] = loss_ref[:step, :]
        me = lax.axis_index(AX)
        bar = pltpu.get_barrier_semaphore()

        def to_others(do):
            def one(k, _):
                do(lax.rem(me + k, NDEV))
                return 0

            lax.fori_loop(1, NDEV, one, 0)

        def scatter(src_of, dst, j):
            to_others(lambda d: pltpu.make_async_remote_copy(
                src_ref=src_of(d), dst_ref=dst, send_sem=ssem.at[j], recv_sem=rsem.at[j],
                device_id=(d,), device_id_type=MESH).start())

        def drain(v, *done):
            for sem in done:
                pltpu.make_async_copy(v, v, sem).wait()

        to_others(lambda d: pl.semaphore_signal(bar, device_id=(d,), device_id_type=MESH))
        pl.semaphore_wait(bar, NDEV - 1)
        others = pl.ds(0, NDEV - 1)
        scatter(lambda d: p_ref.at[d, told], got.at[me, told], 0)
        scatter(lambda d: p_ref.at[d, kept], got.at[me, kept], 1)
        own = pltpu.make_async_copy(p_ref.at[me], got.at[me], lsem.at[0])
        own.start()
        own.wait()
        drain(got.at[others, told], rsem.at[0])
        mine[...] = total([got[d, told] for d in range(NDEV)])
        drain(got.at[others, told], ssem.at[0])
        scatter(lambda d: mine, all_ref.at[me], 2)
        keep = pltpu.make_async_copy(mine, all_ref.at[me], lsem.at[1])
        keep.start()
        keep.wait()
        drain(got.at[others, kept], rsem.at[1], ssem.at[1])
        own_ref[...] = total([got[d, kept] for d in range(NDEV)])
        drain(all_ref.at[others], rsem.at[2], ssem.at[2])

    dma = pltpu.SemaphoreType.DMA
    vm = pl.BlockSpec(memory_space=VMEM)
    told_rows = jax.ShapeDtypeStruct((NDEV, told.size, D), F32)
    return pl.pallas_call(
        kernel, name='reduce_shares',
        out_shape=[jax.ShapeDtypeStruct((kept.size, D), F32), told_rows],
        in_specs=[vm] * (n + 1), out_specs=[vm, vm],
        scratch_shapes=[VMEM((NDEV, RED, D), F32)] * 2 + [VMEM((told.size, D), F32), dma((3,)), dma((3,)), dma((2,))],
        compiler_params=pltpu.CompilerParams(collective_id=cid, has_side_effects=True))(*grads, loss)


def lay_out(own, every):
    step = D // NDEV

    def kernel(own_ref, all_ref, loss_ref, self1, nbr1, self2, nbr2, self3, nbr3, last):
        self1[...], nbr1[...] = own_ref[:step, :], own_ref[step:, :]
        for d in range(NDEV):
            for j, out in enumerate((self2, nbr2, last)):
                out[d * step:(d + 1) * step, :] = all_ref[d, j * step:(j + 1) * step, :]
        turned = last[...].T
        self3[...], nbr3[...] = turned[:C], turned[D // 2:D // 2 + C]
        loss_ref[...] = all_ref[0, 3 * step:3 * step + 1, :1] / N

    shapes = [(1, 1), (step, D), (step, D), (D, D), (D, D), (C, D), (C, D)]
    return pl.pallas_call(
        kernel, name='lay_out', out_shape=[jax.ShapeDtypeStruct(v, F32) for v in shapes],
        scratch_shapes=[VMEM((D, D), F32)])(own, every)


def solution(mesh):
    def device_step(feat_cols, w_self1_rows, w_nbr1_rows, nbr_rows, mask_rows, w_self2, w_nbr2, w_self3, w_nbr3, label_rows):
        me = lax.axis_index(AX)
        live = mask_rows.T > 0
        ids = rank(nbr_rows.T)
        w1_rows = jnp.concatenate([w_self1_rows, w_nbr1_rows], axis=1)
        out_going = jnp.concatenate(
            [feat_cols.T.reshape(4, 16, NDEV, 128).transpose(2, 0, 1, 3).reshape(NDEV, 4, R),
             jnp.broadcast_to(w1_rows[None], (NDEV, 4, 2 * D))], axis=2)
        in_coming = lax.all_to_all(out_going, AX, 0, 0, tiled=True)
        edges = sorted_edges(ids, live)
        rows = jnp.concatenate([jnp.where(live, ids, N), label_rows[None, :], jnp.zeros((5, R), jnp.int32)])
        blocks = rows.reshape(16, 16, 128).transpose(1, 0, 2)
        blocks = lax.all_to_all(jnp.concatenate([blocks, blocks]), AX, 0, 0, tiled=True)
        rows = lax.dynamic_index_in_dim(blocks.reshape(16, 2, 16, 128), me // 16, 1, keepdims=False)
        rows = rows.transpose(1, 0, 2).reshape(16, R)
        idx, labels = rows[:K], rows[K]
        in_coming = in_coming.reshape(D, R + 2 * D)
        feat = in_coming[:, :R].T
        w_self1, w_nbr1 = in_coming[:, R:R + D], in_coming[:, R + D:]
        deg = jnp.sum((idx < N).astype(F32), axis=0)
        side = jnp.stack([deg, labels.astype(F32)], axis=1)
        idx = idx.reshape(E)
        halves = lambda w: jnp.stack([jnp.pad(w, ((0, 0), (0, D - C))), jnp.pad(w, ((0, 0), (D // 2, D // 2 - C)))])
        ws3, wn3 = halves(w_self3), halves(w_nbr3)
        wn3_t = jnp.concatenate([wn3[0], wn3[1]]).T
        agg_x, pre_one, act_one = hidden_layer(feat, idx, side, w_self1, w_nbr1)
        agg_one, pre_two, act_two = hidden_layer(act_one, idx, side, w_self2, w_nbr2)
        g_three, dws3, dwn3, loss = output_layer(act_two, idx, side, ws3, wn3)
        packed, edges = all_gather([g_three, edges], PACKED_CHUNKS, PACKED_ORDER, 5, VLIM)
        lists = in_edges(edges)
        g_two, u_one, dws2, dwn2 = backward_layer(
            packed, None, edges, lists, g_three, ws3, pre_two, act_one, agg_one, w_nbr2, wn3_t)
        dws1, dwn1 = backward_layer(
            packed, gather_rows(u_one), edges, lists, g_two, w_self2, pre_one, feat, agg_x, None, None)
        last = jnp.concatenate([v[:, :D // 2] + v[:, D // 2:] for v in (dws3, dwn3)], axis=1)
        loss, *firsts, last_self, last_nbr = lay_out(*reduce_shares([dws1, dwn1, dws2, dwn2, last], loss, 7))
        return (loss.reshape(()), *firsts, last_self.T, last_nbr.T)

    row = P(AX, None)
    return jax.shard_map(
        device_step, mesh=mesh,
        in_specs=(P(None, AX), row, row, row, row, P(), P(), P(), P(), P(AX)),
        out_specs=(P(), row, row, P(), P(), P(), P()),
        check_vma=False)
```

```python
import jax
import jax.numpy as jnp
from jax import lax
from jax.experimental import pallas as pl
from jax.experimental.pallas import tpu as pltpu
from jax.sharding import PartitionSpec as P


AX = 'g'
N = 65536
R = 2048
D = 128
K = 10
C = 40
NDEV = 32
E = R * K
CAP = 2048
NACC = 8
EDGES = 64
SLOTS = 8
TBUF = 10
BBUF = 8
UNROLL = 64
MESH = pl.DeviceIdType.MESH
VMEM = pltpu.VMEM
BF = jnp.bfloat16
F32 = jnp.float32
VLIM = 62 * 1024 * 1024
BLIM = 53 * 1024 * 1024
LLIM = 46 * 1024 * 1024
GLIM = 48 * 1024 * 1024


def gather_blocks(arrays, chunks, order, lsem, rsem, sems):
    nq = len(chunks)
    me = lax.axis_index(AX)
    z, y, x, c = me // 8, lax.rem(me // 4, 2), lax.rem(me // 2, 2), lax.rem(me, 2)

    def dev(z_, y_, x_, c_):
        return ((z_ * 2 + y_) * 2 + x_) * 2 + c_

    d_x, d_y, d_up, d_dn, d_c = dev(z, y, 1 - x, c), dev(z, 1 - y, x, c), me + 8, me - 8, dev(z, y, x, 1 - c)
    bar = pltpu.get_barrier_semaphore()
    for d in (d_x, d_y, d_c):
        pl.semaphore_signal(bar, device_id=(d,), device_id_type=MESH)

    @pl.when(z < 3)
    def _():
        pl.semaphore_signal(bar, device_id=(d_up,), device_id_type=MESH)

    @pl.when(z > 0)
    def _():
        pl.semaphore_signal(bar, device_id=(d_dn,), device_id_type=MESH)

    pl.semaphore_wait(bar, 4 + lax.rem(z + 1, 4) // 2)
    sent = [[[0] for _ in range(4)] for _ in arrays]

    def place(q, zo, yo, xo):
        array, first, rows, _ = chunks[q]
        block, table = arrays[array]
        return table.at[pl.ds(pl.multiple_of(dev(zo, yo, xo, c) * block.shape[0] + first, 8), rows)]

    def slot(q, zo, yo, xo):
        return rsem.at[((zo * 2 + yo) * 2 + xo) * nq + q]

    def forward(q, zo, yo, xo, up, dn, to_x, to_y, src=None):
        dst = place(q, zo, yo, xo)
        src = dst if src is None else src
        ssem, csem = sems[chunks[q][0]]

        def send(d, ss, rs):
            pltpu.make_async_remote_copy(
                src_ref=src, dst_ref=dst, send_sem=ss, recv_sem=rs, device_id=(d,), device_id_type=MESH).start()

        if up is not None:
            @pl.when(up)
            def _():
                send(d_up, ssem.at[0], slot(q, zo, yo, xo))

            @pl.when(dn)
            def _():
                send(d_dn, ssem.at[1], slot(q, zo, yo, xo))
        for there, d, j in ((to_x, d_x, 2), (to_y, d_y, 3)):
            if there:
                send(d, ssem.at[j], slot(q, zo, yo, xo))
                sent[chunks[q][0]][j][0] += chunks[q][2]
        send(d_c, csem.at[0], csem.at[1])

    own = []
    for q in order[:nq]:
        array, first, rows, _ = chunks[q]
        forward(q, z, y, x, z < 3, z > 0, True, True, arrays[array][0].at[pl.ds(first, rows)])
    for j, (block, table) in enumerate(arrays):
        rb = block.shape[0]
        own.append(pltpu.make_async_copy(block, table.at[pl.ds(pl.multiple_of(me * rb, 8), rb)], lsem.at[j]))
        own[j].start()
    zr = [z, z + 1 - 2 * lax.rem(z, 2), 2 - z // 2, 3 - 3 * (z // 2)]

    for code in order[nq:]:
        kind, r, q = code // 100, code // 10 % 10, code % 10
        plane_first = chunks[q][3]
        zo, yo, xo = zr[r], 1 - y if kind >= 2 else y, 1 - x if kind % 2 else x
        here = place(q, zo, yo, xo)
        pltpu.make_async_remote_copy(
            src_ref=here, dst_ref=here, send_sem=sems[0][0].at[0], recv_sem=slot(q, zo, yo, xo),
            device_id=(d_x,), device_id_type=MESH).wait_recv()
        up = dn = None
        if kind == 0 or plane_first:
            up, dn = (z < 3, z > 0) if r == 0 else ((zo < z) & (z < 3), (zo > z) & (z > 0))
        column = kind == 0 and not plane_first
        across = not plane_first or r == 0
        forward(q, zo, yo, xo, up, dn,
                column or (kind == 2 and q % 2 == 1 and across), column or (kind == 1 and q % 2 == 0 and across))

    for j, (block, table) in enumerate(arrays):
        ssem, csem = sems[j]

        def wait_rows(n, sem, table=table):
            v = table.at[pl.ds(0, n)]
            pltpu.make_async_copy(v, v, sem).wait()

        own[j].wait()
        for k in (2, 3):
            wait_rows(sent[j][k][0], ssem.at[k])
        step = sum(rows * (4 if plane_first else 1) for array, _, rows, plane_first in chunks if array == j)
        for k in range(3):
            @pl.when(z == k)
            def _(k=k):
                wait_rows((k + 1) * step, ssem.at[0])

            @pl.when(z == 3 - k)
            def _(k=k):
                wait_rows((k + 1) * step, ssem.at[1])
        wait_rows(16 * block.shape[0], csem.at[0])
        wait_rows(16 * block.shape[0], csem.at[1])


def cut(*sizes, array=0, plane_first=0):
    return [(array, sum(sizes[:i]), n, i < plane_first) for i, n in enumerate(sizes)]


def steps(*words):
    every = [w // 1000 ** i % 1000 for w in words for i in reversed(range(8))]
    return [v for v in every if v != 999]


ROW_CHUNKS = cut(224, 224, 272, 272, 272, 272, 256, 256, plane_first=2)
ROW_ORDER = steps(
    2003006005000004001007, 14100013201206200204016, 12017027023207101116026, 25015036111032033034211,
    24035021213020115215106, 300110022037220125126205, 104225320113112316120136, 224102217130310203011124,
    301227234114235105132237, 135307313212122010236117, 31134210107123216315121, 202223131103127306321311,
    304030317233133222312232, 137221231326331226230302, 303214305330336332322333, 323337325335314327334324)
PACKED_CHUNKS = cut(144, 144, 128, 128, 128, 128, 112, 112, plane_first=2) + cut(88, 80, array=1)
PACKED_TURNS = [8, 9, *range(8)]
PACKED_ORDER = PACKED_TURNS + [
    kind * 100 + (s + step) * 10 + q for s in range(5) for q in PACKED_TURNS
    for kind, step in ((0, 1), (1, 0), (2, 0), (3, -1)) if 0 <= s + step <= 3]


def all_gather(blocks, chunks, order, cid, limit):
    n = len(blocks)

    def kernel(*refs):
        lsem, rsem, *sems = refs[2 * n:]
        gather_blocks(list(zip(refs[:n], refs[n:2 * n])), chunks, order, lsem, rsem, list(zip(sems[::2], sems[1::2])))

    dma = pltpu.SemaphoreType.DMA
    return pl.pallas_call(
        kernel, out_shape=[jax.ShapeDtypeStruct((v.shape[0] * NDEV,) + v.shape[1:], v.dtype) for v in blocks],
        in_specs=[pl.BlockSpec(memory_space=VMEM)] * n, out_specs=[pl.BlockSpec(memory_space=pltpu.HBM)] * n,
        scratch_shapes=[dma((n,)), dma((16 * len(chunks),))] + [dma((4,)), dma((2,))] * n,
        compiler_params=pltpu.CompilerParams(
            collective_id=cid, has_side_effects=True, vmem_limit_bytes=limit))(*blocks)


def gather_rows(v):
    return all_gather([v], ROW_CHUNKS, ROW_ORDER, 2, GLIM)[0]


def dot(a, b):
    return jnp.dot(a, b, preferred_element_type=F32)


def dot_rows(a, b):
    return lax.dot_general(a, b, (((0,), (0,)), ((), ())), preferred_element_type=F32)


def dot_t(a, b):
    return lax.dot_general(a, b, (((1,), (1,)), ((), ())), preferred_element_type=F32)


CB = 256


def load_table(sources, make, meanwhile=None):
    slots = sources[0][1].shape[0]

    def copies(i, slot):
        for table, space, sem in sources:
            n = space.shape[1]
            rows = table.at[pl.ds(pl.multiple_of(i * n, n), n), :]
            yield pltpu.make_async_copy(rows, space.at[slot], sem.at[slot])

    for i in range(slots - 1):
        for copy in copies(i, i):
            copy.start()
    if meanwhile is not None:
        meanwhile()

    def step(i, _):
        slot = lax.rem(i, slots)
        for copy in copies(i, slot):
            copy.wait()

        @pl.when(i + slots - 1 < NDEV)
        def _():
            for copy in copies(i + slots - 1, lax.rem(i + slots - 1, slots)):
                copy.start()

        make(i, slot)
        return 0

    lax.fori_loop(0, NDEV, step, 0)


class Inputs:
    def __init__(self, operands, spaces, sem):
        self.copies = [pltpu.make_async_copy(a, b, sem.at[j]) for j, (a, b) in enumerate(zip(operands, spaces))]

    def start(self):
        for copy in self.copies:
            copy.start()


def table_mean(tab_hbm, inputs, idx_ref, tab, stg, acc, tsem):
    def widen(i, slot):
        tab[pl.ds(pl.multiple_of(i * R, R), R), :] = stg[slot].astype(F32)

    load_table([(tab_hbm, stg, tsem)], widen, inputs.start)
    tab[pl.ds(N, 8), :] = jnp.zeros((8, D), F32)
    inputs.copies[0].wait()
    slots = [idx_ref.at[pl.ds(k * R, R)] for k in range(K)]

    def body(b, _):
        for u in range(UNROLL):
            r = b * UNROLL + u
            acc[pl.ds(r, 1), :] = total([tab[pl.ds(ids[r], 1), :] for ids in slots])
        return 0

    lax.fori_loop(0, R // UNROLL, body, 0)
    for copy in inputs.copies[1:]:
        copy.wait()


TABLE = [VMEM((N + 8, D), F32), VMEM((TBUF, R, D), BF), VMEM((R, D), F32), pltpu.SemaphoreType.DMA((TBUF,)),
         pltpu.SMEM((E,), jnp.int32), VMEM((R, D), BF), VMEM((R, 2), F32), pltpu.SemaphoreType.DMA((3,))]
HBM = pl.BlockSpec(memory_space=pltpu.HBM)


def hidden_layer(v, idx, side, w_self, w_nbr):
    def kernel(idx_hbm, tab_hbm, x_hbm, side_hbm, ws_ref, wn_ref, agg_ref, pre_ref, act_ref,
               tab, stg, acc, tsem, idx_ref, x_ref, side_ref, sem):
        inputs = Inputs((idx_hbm, x_hbm, side_hbm), (idx_ref, x_ref, side_ref), sem)
        table_mean(tab_hbm, inputs, idx_ref, tab, stg, acc, tsem)

        def block(i, _):
            r = pl.ds(pl.multiple_of(i * CB, CB), CB)
            agg = (acc[r, :] / side_ref[r, :1]).astype(BF)
            agg_ref[r, :] = agg
            pre = dot(x_ref[r, :], ws_ref[...]) + dot(agg, wn_ref[...])
            pre_ref[r, :] = pre
            act_ref[r, :] = jnp.maximum(pre, 0.0).astype(BF)
            return 0

        lax.fori_loop(0, R // CB, block, 0)

    vm = pl.BlockSpec(memory_space=VMEM)
    return pl.pallas_call(
        kernel,
        out_shape=[jax.ShapeDtypeStruct((R, D), BF), jax.ShapeDtypeStruct((R, D), F32), jax.ShapeDtypeStruct((R, D), BF)],
        in_specs=[HBM] * 4 + [vm] * 2,
        out_specs=[vm] * 3, scratch_shapes=TABLE, compiler_params=pltpu.CompilerParams(vmem_limit_bytes=LLIM),
    )(idx, gather_rows(v), v, side, w_self, w_nbr)


HALF = R // 2


def output_layer(v, idx, side, w_self, w_nbr):
    def kernel(idx_hbm, tab_hbm, x_hbm, side_hbm, ws_ref, wn_ref, g_ref, dws_ref, dwn_ref, loss_ref,
               tab, stg, acc, tsem, idx_ref, x_ref, side_ref, sem):
        inputs = Inputs((idx_hbm, x_hbm, side_hbm), (idx_ref, x_ref, side_ref), sem)
        table_mean(tab_hbm, inputs, idx_ref, tab, stg, acc, tsem)
        dws_ref[...] = jnp.zeros((D, D), F32)
        dwn_ref[...] = jnp.zeros((D, D), F32)
        lane = lax.broadcasted_iota(jnp.int32, (CB, D), 1)

        def part(start, half):
            r = pl.ds(pl.multiple_of(start, CB), CB)
            act = x_ref[r, :]
            agg = (acc[r, :] / side_ref[r, :1]).astype(BF)
            logits = dot(act, ws_ref[half]) + dot(agg, wn_ref[half])
            col = lane - half * (D // 2)
            live = (col >= 0) & (col < C)
            top = jnp.max(jnp.where(live, logits, -jnp.inf), axis=1, keepdims=True)
            ex = jnp.where(live, jnp.exp(logits - top), 0.0)
            norm = top + jnp.log(jnp.sum(ex, axis=1, keepdims=True))
            hot = jnp.where(col.astype(F32) == side_ref[r, 1:], 1.0, 0.0)
            loss = jnp.sum(jnp.where(live, hot * (norm - logits), 0.0))
            prob = jnp.where(live, jnp.exp(logits - norm), 0.0)
            g = ((prob - hot) / N).astype(BF)
            dws_ref[...] += dot_rows(act, g)
            dwn_ref[...] += dot_rows(agg, g)
            rest = 1.0 / side_ref[r, :1]
            for j in range(3):
                most = rest.astype(BF)
                g = jnp.where(col == C + j, most, g)
                rest = rest - most.astype(F32)
            return g, loss

        def block(i, loss):
            g_low, loss_low = part(i * CB, 0)
            g_high, loss_high = part(i * CB + HALF, 1)
            g_ref[pl.ds(pl.multiple_of(i * CB, CB), CB), :] = jnp.where(lane < D // 2, g_low, g_high)
            return loss + loss_low + loss_high

        loss = lax.fori_loop(0, HALF // CB, block, jnp.float32(0.0))
        loss_ref[...] = jnp.full((8, D), loss, F32)

    vm = pl.BlockSpec(memory_space=VMEM)
    return pl.pallas_call(
        kernel,
        out_shape=[jax.ShapeDtypeStruct((HALF, D), BF), jax.ShapeDtypeStruct((D, D), F32),
                   jax.ShapeDtypeStruct((D, D), F32), jax.ShapeDtypeStruct((8, D), F32)],
        in_specs=[HBM] * 4 + [vm] * 2,
        out_specs=[vm] * 4, scratch_shapes=TABLE, compiler_params=pltpu.CompilerParams(vmem_limit_bytes=LLIM),
    )(idx, gather_rows(v), v, side, w_self, w_nbr)


def table_mean_t(fetch, marks, lists_hbm, lists, lsem, tab, accs, load, inputs):
    me = lax.axis_index(AX)

    def base_of(s):
        return jnp.minimum(marks[s, me] // 1024, (SPAN - CAP) // 1024) * 1024

    def list_copies(s, part, slot):
        off = pl.multiple_of(s * SPAN + base_of(s) + part * CAP, 1024)
        return [pltpu.make_async_copy(h.at[pl.ds(off, CAP)], b.at[pl.ds(pl.multiple_of(slot * CAP, CAP), CAP)], lsem.at[j, slot])
                for j, (h, b) in enumerate(zip(lists_hbm, lists))]

    def clear():
        inputs.start()
        for a in accs:
            a[...] = jnp.zeros(a.shape, F32)
        fetch.wait()
        for s in range(SLOTS - 1):
            for cp in list_copies(s, 0, s):
                cp.start()

    load(clear)
    src, dst = [[v.at[pl.ds(u, SLOTS * CAP - EDGES + 1)] for u in range(EDGES)] for v in lists]

    def run(slot, first, last):
        def body(b, _):
            e = slot * CAP + b * EDGES
            for u in range(EDGES):
                d = pl.ds(dst[u][e], 1)
                accs[u % NACC][d, :] += tab[pl.ds(src[u][e], 1), :]
            return 0

        lax.fori_loop(first // EDGES, (last + EDGES - 1) // EDGES, body, 0)

    def sender(s, _):
        slot = lax.rem(s, SLOTS)
        for cp in list_copies(s, 0, slot):
            cp.wait()

        @pl.when(s + SLOTS - 1 < NDEV)
        def _():
            for cp in list_copies(s + SLOTS - 1, 0, lax.rem(s + SLOTS - 1, SLOTS)):
                cp.start()

        base = base_of(s)
        end = marks[s, me + 1] - base
        run(slot, marks[s, me] - base, jnp.minimum(end, CAP))

        def more(p, _):
            for cp in list_copies(s, p, slot):
                cp.start()
            for cp in list_copies(s, p, slot):
                cp.wait()
            run(slot, 0, jnp.minimum(end - p * CAP, CAP))
            return 0

        lax.fori_loop(1, (end + CAP - 1) // CAP, more, 0)
        return 0

    lax.fori_loop(0, NDEV, sender, 0)
    for copy in inputs.copies:
        copy.wait()


def backward_layer(packed, table, edges, lists, g_up, w_self, pre, act, agg, w_nbr, w_up):
    last = table is not None

    def kernel(edges_hbm, src_hbm, dst_hbm, packed_hbm, gu_hbm, pre_hbm, act_hbm, agg_hbm, ws_ref, *rest):
        if last:
            table_hbm, dws_ref, dwn_ref = rest[:3]
            rest = rest[3:]
        else:
            wn_ref, wu_ref, g_ref, u_ref, dws_ref, dwn_ref = rest[:6]
            rest = rest[6:]
        accs, rest = rest[:NACC], rest[NACC:]
        marks, src, dst, lsem, tab, spread, gu_ref, pre_ref, act_ref, agg_ref, sem, pstg, psem, *rest = rest
        inputs = Inputs((gu_hbm, pre_hbm, act_hbm, agg_hbm), (gu_ref, pre_ref, act_ref, agg_ref), sem)
        fetch = pltpu.make_async_copy(edges_hbm.at[:, E // D, :], marks, sem.at[4])
        fetch.start()

        part_row = lax.broadcasted_iota(jnp.int32, (D, 2 * D), 0) - C
        part_row -= jnp.where(lax.broadcasted_iota(jnp.int32, (D, 2 * D), 1) < D, 0, D // 2)
        spread[...] = jnp.where((part_row >= 0) & (part_row < 3), 1.0, 0.0).astype(BF)

        def make(i, slot):
            for q in range(HALF // CB):
                part = pstg[slot, q * CB:(q + 1) * CB, :]
                scale = dot(part, spread[...])
                if not last:
                    v = dot(part, wu_ref[...]).astype(BF)
                for half in range(2):
                    at = half * HALF + q * CB
                    lanes = slice(half * D, (half + 1) * D)
                    term = rest[0][slot, at:at + CB, :] if last else v[:, lanes]
                    tab[pl.ds(pl.multiple_of(i * R + at, CB), CB), :] = term.astype(F32) * scale[:, lanes]

        sources = [(packed_hbm, pstg, psem)] + ([(table_hbm, *rest)] if last else [])
        table_mean_t(fetch, marks, (src_hbm, dst_hbm), (src, dst), lsem, tab, accs,
                     lambda clear: load_table(sources, make, clear), inputs)
        dws_ref[...] = jnp.zeros((D, D), F32)
        dwn_ref[...] = jnp.zeros((D, D), F32)

        def part(start, up):
            r = pl.ds(pl.multiple_of(start, CB), CB)
            g = jnp.where(pre_ref[r, :] > 0, up + total([a[r, :] for a in accs]), 0.0).astype(BF)
            dws_ref[...] += dot_rows(act_ref[r, :], g)
            dwn_ref[...] += dot_rows(agg_ref[r, :], g)
            if not last:
                g_ref[r, :] = g
                u_ref[r, :] = dot_t(g, wn_ref[...]).astype(BF)

        def block(i, _):
            if last:
                part(i * CB, dot_t(gu_ref[pl.ds(pl.multiple_of(i * CB, CB), CB), :], ws_ref[...]))
            else:
                gu = gu_ref[pl.ds(pl.multiple_of(i * CB, CB), CB), :]
                part(i * CB, dot_t(gu, ws_ref[0]))
                part(i * CB + HALF, dot_t(gu, ws_ref[1]))
            return 0

        lax.fori_loop(0, (R if last else HALF) // CB, block, 0)

    vm = pl.BlockSpec(memory_space=VMEM)
    outs = [jax.ShapeDtypeStruct((D, D), F32)] * 2
    args = [edges.reshape(NDEV, SPAN // D, D), *lists, packed, g_up, pre, act, agg, w_self]
    specs = [HBM] * 8 + [vm]
    stage = [VMEM((BBUF, HALF, D), BF), pltpu.SemaphoreType.DMA((BBUF,))]
    if last:
        args.append(table)
        specs.append(HBM)
        stage += [VMEM((BBUF, R, D), BF), pltpu.SemaphoreType.DMA((BBUF,))]
    else:
        outs = [jax.ShapeDtypeStruct((R, D), BF)] * 2 + outs
        args += [w_nbr, w_up]
        specs += [vm, vm]
    return pl.pallas_call(
        kernel, out_shape=outs, in_specs=specs, out_specs=[vm] * len(outs),
        scratch_shapes=[VMEM((R + 8, D), F32)] * NACC + [pltpu.SMEM((NDEV, D), jnp.int32)] + [pltpu.SMEM((SLOTS * CAP,), jnp.int32)] * 2
        + [pltpu.SemaphoreType.DMA((2, SLOTS)), VMEM((N, D), F32), VMEM((D, 2 * D), BF)]
        + [VMEM(v.shape, v.dtype) for v in (g_up, pre, act, agg)] + [pltpu.SemaphoreType.DMA((5,))] + stage,
        compiler_params=pltpu.CompilerParams(vmem_limit_bytes=BLIM))(*args)


def rank(j):
    return ((j >> 7) & (NDEV - 1)) * R + (j >> 12) * 128 + (j & 127)


SPAN = 21 * 1024


def sorted_edges(ids, live):
    here = jnp.arange(R, dtype=jnp.int32)[None, :]
    key = jnp.where(live, ids * R + here, -1)
    key = lax.sort(key.reshape(E))
    bounds = jnp.arange(NDEV + 1, dtype=jnp.int32)
    starts = jnp.sum(((key >> 22)[None, :] < bounds[:, None]).astype(jnp.int32), axis=1)
    return jnp.concatenate([key.reshape(E // D, D), jnp.pad(starts[None, :], ((0, 7), (0, D - NDEV - 1)))])


def in_edges(every):
    me = lax.axis_index(AX)
    keys = every.reshape(NDEV, SPAN // D, D)
    sender = jnp.arange(NDEV, dtype=jnp.int32)[:, None, None]
    src = rank(sender * R + (keys & (R - 1)))
    dst = (keys >> 11) - me * R
    real = (dst >= 0) & (dst < R) & (keys >= 0) & (jnp.arange(SPAN // D)[None, :, None] < E // D)
    dst = jnp.where(real, dst, R)
    return src.reshape(-1), dst.reshape(-1)


RED = 24


def total(v):
    while len(v) > 1:
        v = [v[j] + v[j + 1] if j + 1 < len(v) else v[j] for j in range(0, len(v), 2)]
    return v[0]


def reduce_shares(grads, loss, cid):
    n = len(grads)
    step = D // NDEV
    kept, told = pl.ds(0, 2 * step), pl.ds(2 * step, RED - 2 * step)

    def kernel(*refs):
        loss_ref, own_ref, all_ref, p_ref, got, mine, rsem, ssem, lsem = refs[n:]
        for d in range(NDEV):
            for j in range(n):
                p_ref[d, j * step:(j + 1) * step, :] = refs[j][d * step:(d + 1) * step, :]
            p_ref[d, n * step:, :] = loss_ref[:step, :]
        me = lax.axis_index(AX)
        bar = pltpu.get_barrier_semaphore()

        def to_others(do):
            def one(k, _):
                do(lax.rem(me + k, NDEV))
                return 0

            lax.fori_loop(1, NDEV, one, 0)

        def scatter(src_of, dst, j):
            to_others(lambda d: pltpu.make_async_remote_copy(
                src_ref=src_of(d), dst_ref=dst, send_sem=ssem.at[j], recv_sem=rsem.at[j],
                device_id=(d,), device_id_type=MESH).start())

        def drain(v, *done):
            for sem in done:
                pltpu.make_async_copy(v, v, sem).wait()

        to_others(lambda d: pl.semaphore_signal(bar, device_id=(d,), device_id_type=MESH))
        pl.semaphore_wait(bar, NDEV - 1)
        others = pl.ds(0, NDEV - 1)
        scatter(lambda d: p_ref.at[d, told], got.at[me, told], 0)
        scatter(lambda d: p_ref.at[d, kept], got.at[me, kept], 1)
        own = pltpu.make_async_copy(p_ref.at[me], got.at[me], lsem.at[0])
        own.start()
        own.wait()
        drain(got.at[others, told], rsem.at[0])
        mine[...] = total([got[d, told] for d in range(NDEV)])
        drain(got.at[others, told], ssem.at[0])
        scatter(lambda d: mine, all_ref.at[me], 2)
        keep = pltpu.make_async_copy(mine, all_ref.at[me], lsem.at[1])
        keep.start()
        keep.wait()
        drain(got.at[others, kept], rsem.at[1], ssem.at[1])
        own_ref[...] = total([got[d, kept] for d in range(NDEV)])
        drain(all_ref.at[others], rsem.at[2], ssem.at[2])

    dma = pltpu.SemaphoreType.DMA
    vm = pl.BlockSpec(memory_space=VMEM)
    told_rows = jax.ShapeDtypeStruct((NDEV, told.size, D), F32)
    return pl.pallas_call(
        kernel, name='reduce_shares',
        out_shape=[jax.ShapeDtypeStruct((kept.size, D), F32), told_rows],
        in_specs=[vm] * (n + 1), out_specs=[vm, vm],
        scratch_shapes=[VMEM((NDEV, RED, D), F32)] * 2 + [VMEM((told.size, D), F32), dma((3,)), dma((3,)), dma((2,))],
        compiler_params=pltpu.CompilerParams(collective_id=cid, has_side_effects=True))(*grads, loss)


def lay_out(own, every):
    step = D // NDEV

    def kernel(own_ref, all_ref, loss_ref, self1, nbr1, self2, nbr2, self3, nbr3, last):
        self1[...], nbr1[...] = own_ref[:step, :], own_ref[step:, :]
        for d in range(NDEV):
            for j, out in enumerate((self2, nbr2, last)):
                out[d * step:(d + 1) * step, :] = all_ref[d, j * step:(j + 1) * step, :]
        turned = last[...].T
        self3[...], nbr3[...] = turned[:C], turned[D // 2:D // 2 + C]
        loss_ref[...] = all_ref[0, 3 * step:3 * step + 1, :1] / N

    shapes = [(1, 1), (step, D), (step, D), (D, D), (D, D), (C, D), (C, D)]
    return pl.pallas_call(
        kernel, name='lay_out', out_shape=[jax.ShapeDtypeStruct(v, F32) for v in shapes],
        scratch_shapes=[VMEM((D, D), F32)])(own, every)


def solution(mesh):
    def device_step(feat_cols, w_self1_rows, w_nbr1_rows, nbr_rows, mask_rows, w_self2, w_nbr2, w_self3, w_nbr3, label_rows):
        me = lax.axis_index(AX)
        live = mask_rows.T > 0
        ids = rank(nbr_rows.T)
        w1_rows = jnp.concatenate([w_self1_rows, w_nbr1_rows], axis=1)
        out_going = jnp.concatenate(
            [feat_cols.T.reshape(4, 16, NDEV, 128).transpose(2, 0, 1, 3).reshape(NDEV, 4, R),
             jnp.broadcast_to(w1_rows[None], (NDEV, 4, 2 * D))], axis=2)
        in_coming = lax.all_to_all(out_going, AX, 0, 0, tiled=True)
        edges = sorted_edges(ids, live)
        rows = jnp.concatenate([jnp.where(live, ids, N), label_rows[None, :], jnp.zeros((5, R), jnp.int32)])
        blocks = rows.reshape(16, 16, 128).transpose(1, 0, 2)
        blocks = lax.all_to_all(jnp.concatenate([blocks, blocks]), AX, 0, 0, tiled=True)
        rows = lax.dynamic_index_in_dim(blocks.reshape(16, 2, 16, 128), me // 16, 1, keepdims=False)
        rows = rows.transpose(1, 0, 2).reshape(16, R)
        idx, labels = rows[:K], rows[K]
        in_coming = in_coming.reshape(D, R + 2 * D)
        feat = in_coming[:, :R].T
        w_self1, w_nbr1 = in_coming[:, R:R + D], in_coming[:, R + D:]
        deg = jnp.sum((idx < N).astype(F32), axis=0)
        side = jnp.stack([deg, labels.astype(F32)], axis=1)
        idx = idx.reshape(E)
        halves = lambda w: jnp.stack([jnp.pad(w, ((0, 0), (0, D - C))), jnp.pad(w, ((0, 0), (D // 2, D // 2 - C)))])
        ws3, wn3 = halves(w_self3), halves(w_nbr3)
        wn3_t = jnp.concatenate([wn3[0], wn3[1]]).T
        agg_x, pre_one, act_one = hidden_layer(feat, idx, side, w_self1, w_nbr1)
        agg_one, pre_two, act_two = hidden_layer(act_one, idx, side, w_self2, w_nbr2)
        g_three, dws3, dwn3, loss = output_layer(act_two, idx, side, ws3, wn3)
        packed, edges = all_gather([g_three, edges], PACKED_CHUNKS, PACKED_ORDER, 5, VLIM)
        lists = in_edges(edges)
        g_two, u_one, dws2, dwn2 = backward_layer(
            packed, None, edges, lists, g_three, ws3, pre_two, act_one, agg_one, w_nbr2, wn3_t)
        dws1, dwn1 = backward_layer(
            packed, gather_rows(u_one), edges, lists, g_two, w_self2, pre_one, feat, agg_x, None, None)
        last = jnp.concatenate([v[:, :D // 2] + v[:, D // 2:] for v in (dws3, dwn3)], axis=1)
        loss, *firsts, last_self, last_nbr = lay_out(*reduce_shares([dws1, dwn1, dws2, dwn2, last], loss, 7))
        return (loss.reshape(()), *firsts, last_self.T, last_nbr.T)

    row = P(AX, None)
    return jax.shard_map(
        device_step, mesh=mesh,
        in_specs=(P(None, AX), row, row, row, row, P(), P(), P(), P(), P(AX)),
        out_specs=(P(), row, row, P(), P(), P(), P()),
        check_vma=False)
```
